256 devices in a mesh: dp: 4 (over x), vocab: 64 (over y, z, core).
Axes of the slice: x: 4, y: 4, z: 8, core: 2. Of those that a mesh axis runs over, the one named last changes fastest.
Arguments:
- final_activation: bfloat16 [512, 8192], P('dp', 'vocab'), may hold values from -2000 to 2000
- output_projection_weights: bfloat16 [8192, 128256], P('dp', 'vocab'), may hold values from -0.0625 to 0.0625
- context_word_tallies: int32 [512, 128256], P('dp', 'vocab'), may hold values from 0 to 2
- emitted_word_tallies: int32 [512, 128256], P('dp', 'vocab'), may hold values from 0 to 2
- freshest_word: int32 [512], P('dp'), may hold values from 0 to 128255
- recurrence_divisor: float32 [512], P('dp'), may hold values from 1.1 to 2.5
- recurrence_fine: float32 [512], P('dp'), may hold values from 0 to 1.5
- appearance_fine: float32 [512], P('dp'), may hold values from 0 to 1.5
- softness_level: float32 [512], P('dp'), may hold values from 0.5 to 2
- random_draws: float32 [512], P('dp'), may hold values from 0.02 to 0.98
Outputs:
- new_counts: int32 [512, 128256], P('dp', 'vocab')
- log_likelihoods: float32 [512, 128256], P('dp', 'vocab')
- sample_quantile: float32 [512], P('dp')
The draws below stay inside these ranges and needn't reach their ends.
All inputs are finite; a program needn't handle non-finite values.
Results may differ from the reference program's by a relative error of at most 0.0012.
Values may be sent and summed in bfloat16 or wider, within the bound.
No kernel may reach another device: no remote copies, remote signals or barrier semaphores. Data moves between devices by JAX's collectives and lax.ppermute only.
A program may use at most 128 MiB of HBM per device.

```python
import math
import jax
import jax.numpy as jnp
from jax import lax

D = 8192
VOCAB = 128256
STREAM_NUMBER = 512
N_VOCAB = 64


def draw_final_activation(key, part):
    values = jnp.clip(jax.random.normal(key, (STREAM_NUMBER, D), jnp.float32), -6.0, 6.0)
    row_ids = lax.broadcasted_iota(jnp.int32, (STREAM_NUMBER, 1), 0)
    values = values * jnp.where(row_ids % 4 == 0, 150.0, 1.0)
    return values.astype(jnp.bfloat16)


def place_ends(array, own_key, smallest, largest):
    longest = array.shape.index(max(array.shape))
    spots = []
    for shift in (0, 1):
        where = [jax.random.randint(jax.random.fold_in(own_key, axis), (), 0, length) for axis, length in enumerate(array.shape)]
        where[longest] = (where[longest] + shift) % array.shape[longest]
        spots.append(tuple(where))
    return array.at[spots[0]].set(smallest).at[spots[1]].set(largest)


def shard_levels(own_key, dims, pieces, low, top_value):
    level, own = 1.0, jax.random.fold_in(own_key, 6)
    for dim, shards_of in pieces:
        draws = jnp.exp(jax.random.uniform(jax.random.fold_in(own, dim), (shards_of,), jnp.float32, low / len(pieces), top_value / len(pieces)))
        level = level * jnp.repeat(draws, dims[dim] // shards_of).reshape([-1 if axis == dim else 1 for axis in range(len(dims))])
    return level


def centred(key, dims, width, limit, pieces=(), kind=jnp.bfloat16):
    gain = shard_levels(key, dims, pieces, -0.22, 0.18) if pieces else 1.0
    entries = jax.random.normal(key, dims, jnp.float32) * width * gain
    return jnp.minimum(jnp.maximum(entries, -limit), limit).astype(kind)


def setup_inputs(seed: int = 0) -> dict:
    arg_keys = jax.random.split(jax.random.key(seed), 11)
    final_activation = draw_final_activation(jax.random.fold_in(arg_keys[10], 71), 0)
    output_projection_weights = centred(arg_keys[1], (D, VOCAB), D ** -0.5, 0.0625, ((0, 4), (1, 64)))
    context_word_tallies = place_ends(jax.random.randint(arg_keys[2], (STREAM_NUMBER, VOCAB), 0, 3), jax.random.fold_in(arg_keys[2], 1), 0, 2).astype(jnp.int32)
    emitted_word_tallies = place_ends(jax.random.randint(arg_keys[3], (STREAM_NUMBER, VOCAB), 0, 3), jax.random.fold_in(arg_keys[3], 1), 0, 2).astype(jnp.int32)
    freshest_word = place_ends(jax.random.randint(arg_keys[4], (STREAM_NUMBER,), 0, VOCAB), jax.random.fold_in(arg_keys[4], 1), 0, VOCAB - 1).astype(jnp.int32)
    recurrence_divisor = jnp.clip(jnp.exp(math.log(2.5) - 0.82098053 * jax.random.uniform(arg_keys[5], (STREAM_NUMBER,), jnp.float32) ** shard_levels(arg_keys[5], (STREAM_NUMBER,), ((0, 4),), -0.2, 0.2)), 1.1, 2.5)
    recurrence_fine = jnp.clip(1.5 * jax.random.uniform(arg_keys[6], (STREAM_NUMBER,), jnp.float32) ** shard_levels(arg_keys[6], (STREAM_NUMBER,), ((0, 4),), -0.2, 0.2), 0.0, 1.5)
    appearance_fine = jnp.clip(1.5 * jax.random.uniform(arg_keys[7], (STREAM_NUMBER,), jnp.float32) ** shard_levels(arg_keys[7], (STREAM_NUMBER,), ((0, 4),), -0.2, 0.2), 0.0, 1.5)
    softness_level = jnp.clip(jnp.exp(math.log(2.0) - 1.3862944 * jax.random.uniform(arg_keys[8], (STREAM_NUMBER,), jnp.float32) ** shard_levels(arg_keys[8], (STREAM_NUMBER,), ((0, 4),), -0.2, 0.2)), 0.5, 2.0)
    random_draws = jnp.clip(0.02 + 0.96000002 * jax.random.uniform(arg_keys[9], (STREAM_NUMBER,), jnp.float32) ** shard_levels(arg_keys[9], (STREAM_NUMBER,), ((0, 4),), -0.2, 0.2), 0.02, 0.98)
    return dict(final_activation=final_activation, output_projection_weights=output_projection_weights, context_word_tallies=context_word_tallies, emitted_word_tallies=emitted_word_tallies, freshest_word=freshest_word, recurrence_divisor=recurrence_divisor, recurrence_fine=recurrence_fine, appearance_fine=appearance_fine, softness_level=softness_level, random_draws=random_draws)


def reference(final_activation, output_projection_weights, context_word_tallies, emitted_word_tallies, freshest_word, recurrence_divisor, recurrence_fine, appearance_fine, softness_level, random_draws):
    block_width = VOCAB // N_VOCAB
    hidden_wide = final_activation.astype(jnp.float32)

    def one_block(index):
        weight_block = lax.dynamic_slice_in_dim(output_projection_weights, index * block_width, block_width, 1).astype(jnp.float32)
        return jnp.dot(hidden_wide, weight_block, preferred_element_type=jnp.float32, precision=lax.Precision.HIGHEST)

    blocks = lax.map(one_block, jnp.arange(N_VOCAB, dtype=jnp.int32))
    logits = jnp.transpose(blocks, (1, 0, 2)).reshape(final_activation.shape[0], VOCAB)
    token_ids = jnp.arange(VOCAB, dtype=jnp.int32)
    new_counts = emitted_word_tallies + (token_ids[None, :] == freshest_word[:, None]).astype(jnp.int32)
    seen = (context_word_tallies + new_counts) > 0
    factor = recurrence_divisor[:, None]
    adjusted_scores = jnp.where(seen, jnp.where(logits > 0, logits / factor, logits * factor), logits)
    adjusted_scores = adjusted_scores - recurrence_fine[:, None] * new_counts.astype(jnp.float32)
    adjusted_scores = adjusted_scores - appearance_fine[:, None] * (new_counts > 0).astype(jnp.float32)
    softened_scores = adjusted_scores / softness_level[:, None]
    highest_score = jnp.max(softened_scores, axis=1, keepdims=True)
    exponentiated_mass = jnp.exp(softened_scores - highest_score)
    normalizer_mass = jnp.sum(exponentiated_mass, axis=1, keepdims=True)
    log_likelihoods = softened_scores - highest_score - jnp.log(normalizer_mass)
    probs = exponentiated_mass / normalizer_mass
    cdf = jnp.cumsum(probs, axis=1)
    below = cdf - probs
    taken = jnp.minimum(jnp.maximum(random_draws[:, None] - below, 0.0), probs)
    position = (token_ids.astype(jnp.float32) + 0.5) / VOCAB
    sample_quantile = jnp.sum(taken * position[None, :], axis=1)
    return new_counts, log_likelihoods, sample_quantile
```

```python
import jax
import jax.numpy as jnp
from jax import lax
from jax.sharding import Mesh
from jax.sharding import PartitionSpec as P

VOCAB = 128256
NX, NY, NZ, NC = 4, 4, 8, 2
PLANE = ("y", "z", "c")
EVERY = ("x", "y", "z", "c")
HALF = 1000


def moved(value, to):
    pairs = []
    for x in range(NX):
        for y in range(NY):
            for z in range(NZ):
                for c in range(NC):
                    tx, ty, tz, tc = to(x, y, z, c)
                    source = ((x * NY + y) * NZ + z) * NC + c
                    target = ((tx % NX * NY + ty % NY) * NZ + tz % NZ) * NC + tc % NC
                    pairs.append((source, target))
    return lax.ppermute(value, EVERY, pairs)


def copies_from(value, axis):
    size = lax.axis_size(axis)
    copies = jnp.broadcast_to(value, (size, *value.shape))
    return lax.all_to_all(copies, axis, split_axis=0, concat_axis=0, tiled=True)


def gathered_quarter(rows):
    mine = moved(rows, lambda x, y, z, c: (y, x, z, c))
    mine = copies_from(mine, "z")
    mine = copies_from(mine, "y")
    other = moved(mine, lambda x, y, z, c: (x, y, z, 1 - c))
    first = lax.axis_index("c") == 0
    both = jnp.stack(
        [jnp.where(first, mine, other), jnp.where(first, other, mine)], axis=2
    )
    return jnp.transpose(both, (0, 3, 1, 2, 4)).reshape(NX, 128, 2048)


def summed_at_owner(part):
    def up(value):
        return moved(value, lambda x, y, z, c: (x + 1, y, z, c))

    def down(value):
        return moved(value, lambda x, y, z, c: (x - 1, y, z, c))

    own, after, far, before = part
    far_a = up(far[:HALF])
    far_b = down(far[HALF:])
    after_b = up(after[HALF:])
    before_a = down(before[:HALF])
    after_a = up(after[:HALF] + far_a)
    before_b = down(before[HALF:] + far_b)
    return jnp.concatenate(
        [own[:HALF] + before_a + after_a, own[HALF:] + after_b + before_b], axis=0
    )


def on_device(
    final_activation,
    output_projection_weights,
    context_word_tallies,
    emitted_word_tallies,
    freshest_word,
    recurrence_divisor,
    recurrence_fine,
    appearance_fine,
    softness_level,
    random_draws,
):
    shard_width = output_projection_weights.shape[1]
    shard = lax.axis_index(PLANE)
    token_ids = shard * shard_width + lax.broadcasted_iota(jnp.int32, (1, shard_width), 1)
    new_counts = emitted_word_tallies + (token_ids == freshest_word[:, None]).astype(jnp.int32)
    seen = context_word_tallies + new_counts > 0

    groups = gathered_quarter(final_activation)
    groups = jnp.roll(groups, -lax.axis_index("x"), axis=0)
    weights = output_projection_weights.T
    part = lax.dot_general(
        weights, groups, (((1,), (2,)), ((), ())), preferred_element_type=jnp.float32
    )
    part = [part[:, k] for k in range(NX)]
    logits = summed_at_owner(part).T

    factor = recurrence_divisor[:, None]
    adjusted = jnp.where(seen, jnp.where(logits > 0, logits / factor, logits * factor), logits)
    adjusted = adjusted - recurrence_fine[:, None] * new_counts.astype(jnp.float32)
    adjusted = adjusted - appearance_fine[:, None] * (new_counts > 0).astype(jnp.float32)
    softened = adjusted / softness_level[:, None]

    local_top = jnp.max(softened, axis=1)
    mass = jnp.exp(softened - local_top[:, None])
    local_sum = jnp.sum(mass, axis=1)
    stats = copies_from(jnp.stack([local_top, local_sum]), PLANE)
    stats = stats.reshape(64, 2, 128)
    top = jnp.max(stats[:, 0], axis=0)
    sums = stats[:, 1] * jnp.exp(stats[:, 0] - top)
    total = jnp.sum(sums, axis=0)
    passed = lax.broadcasted_iota(jnp.int32, (64, 1), 0) < shard
    lower = jnp.sum(jnp.where(passed, sums, 0.0), axis=0) / total

    log_likelihoods = softened - top[:, None] - jnp.log(total)[:, None]
    probs = jnp.exp(softened - top[:, None]) / total[:, None]
    below = lower[:, None] + jnp.cumsum(probs, axis=1) - probs
    taken = jnp.minimum(jnp.maximum(random_draws[:, None] - below, 0.0), probs)
    position = (token_ids.astype(jnp.float32) + 0.5) / VOCAB
    partial_quantile = jnp.sum(taken * position, axis=1)
    sample_quantile = jnp.sum(copies_from(partial_quantile[None], PLANE), axis=0)[0]
    return new_counts, log_likelihoods, sample_quantile


def solution(mesh):
    split = Mesh(mesh.devices.reshape(NX, NY, NZ, NC), EVERY)
    whole = P("x", PLANE)
    row = P("x")
    return jax.shard_map(
        on_device,
        mesh=split,
        in_specs=(whole, whole, whole, whole, row, row, row, row, row, row),
        out_specs=(whole, whole, row),
        check_vma=False,
    )
```

```python
import jax
import jax.numpy as jnp
from jax import lax
from jax.experimental import pallas as pl
from jax.experimental.pallas import tpu as pltpu
from jax.sharding import Mesh
from jax.sharding import PartitionSpec as P


VOCAB = 128256
NX, NY, NZ, NC = 4, 4, 8, 2
PLANE = ("y", "z", "c")
EVERY = ("x", "y", "z", "c")

ROWS = 2004
LANES = 128
DEPTH = 2048
HALF = 1008
THIRD = HALF // 3
CHUNK = 56
STEPS = THIRD // CHUNK
BLOCKS = ((0, 256), (256, 512), (768, 512), (1280, ROWS - 1280))
CODED = 2 * THIRD + 8
BITS = 20

WHOLE = pl.BlockSpec(memory_space=pltpu.VMEM)


def moved(value, to):
    pairs = []
    for x in range(NX):
        for y in range(NY):
            for z in range(NZ):
                for c in range(NC):
                    tx, ty, tz, tc = to(x, y, z, c)
                    source = ((x * NY + y) * NZ + z) * NC + c
                    target = ((tx % NX * NY + ty % NY) * NZ + tz % NZ) * NC + tc % NC
                    pairs.append((source, target))
    return lax.ppermute(value, EVERY, pairs)


def up(value):
    return moved(value, lambda x, y, z, c: (x + 1, y, z, c))


def down(value):
    return moved(value, lambda x, y, z, c: (x - 1, y, z, c))


def copies_from(value, axis):
    size = lax.axis_size(axis)
    copies = jnp.broadcast_to(value, (size, *value.shape))
    return lax.all_to_all(copies, axis, split_axis=0, concat_axis=0, tiled=True)


def exchanged(copies):
    return lax.all_to_all(copies, PLANE, split_axis=0, concat_axis=0, tiled=True)


def coded(load, out_ref):
    def largest(j, top):
        for third in range(3):
            part = jnp.abs(load(third * THIRD + j * CHUNK))
            top = jnp.maximum(top, jnp.max(part.reshape(CHUNK // 8, 8, LANES), axis=0))
        return top

    top = lax.fori_loop(0, STEPS, largest, jnp.zeros((8, LANES), jnp.float32))
    top = jnp.maximum(jnp.max(top, axis=0, keepdims=True), 1e-30)
    exponent = jnp.ceil(4.0 * jnp.log2(top))
    scale = jnp.exp2(BITS - 0.25 * exponent)
    limit = float(2**BITS - 1)

    def put(j, carry):
        def whole(third):
            value = jnp.round(load(third * THIRD + j * CHUNK) * scale)
            return jnp.clip(value, -limit, limit).astype(jnp.int32)

        a, b, c = whole(0), whole(1), whole(2)
        mask = (1 << 21) - 1
        out_ref[pl.ds(pl.multiple_of(j * CHUNK, 8), CHUNK), :] = (a & mask) | (c << 21)
        out_ref[pl.ds(pl.multiple_of(THIRD + j * CHUNK, 8), CHUNK), :] = (b & mask) | ((c >> 11) << 21)
        return carry

    lax.fori_loop(0, STEPS, put, 0)
    out_ref[2 * THIRD :, :] = jnp.broadcast_to(exponent.astype(jnp.int32), (8, LANES))


def step_of(ref):
    return jnp.exp2(0.25 * ref[2 * THIRD : 2 * THIRD + 1, :].astype(jnp.float32) - BITS)


def decoded(ref, step, j):
    one = ref[pl.ds(pl.multiple_of(j * CHUNK, 8), CHUNK), :]
    two = ref[pl.ds(pl.multiple_of(THIRD + j * CHUNK, 8), CHUNK), :]
    a = (one << 11) >> 11
    b = (two << 11) >> 11
    c = ((two >> 21) << 11) | ((one >> 21) & 2047)
    return [value.astype(jnp.float32) * step for value in (a, b, c)]


def aligned(start):
    return pl.multiple_of(start, 8)


def shard_index():
    return (lax.axis_index("y") * NZ + lax.axis_index("z")) * NC + lax.axis_index("c")


def product_kernel(
    mine, other, source, far_a, far_b, after_b, before_a, after_a, before_b, own, weights, rows, part, here
):
    copies = [
        pltpu.make_async_copy(source.at[pl.ds(start, size)], weights.at[pl.ds(start, size)], here.at[n])
        for n, (start, size) in enumerate(BLOCKS)
    ]
    for copy in copies:
        copy.start()
    x, c = lax.axis_index("x"), lax.axis_index("c")
    for r in range(NX):
        group = lax.rem(x + r, NX)
        for z in range(NZ):
            at = pl.ds(r * LANES, LANES)
            rows[at, pl.ds(pl.multiple_of((2 * z + c) * 128, 128), 128)] = mine[group, z]
            rows[at, pl.ds(pl.multiple_of((2 * z + 1 - c) * 128, 128), 128)] = other[group, z]

    for (start, size), copy in zip(BLOCKS, copies):
        copy.wait()
        part[pl.ds(start, size), :] = lax.dot_general(
            weights[pl.ds(start, size), :],
            rows[...],
            (((1,), (1,)), ((), ())),
            preferred_element_type=jnp.float32,
        )
    part[ROWS : 2 * HALF, :] = jnp.zeros((2 * HALF - ROWS, NX * LANES), jnp.float32)

    def load(r, half):
        return lambda start: part[pl.ds(aligned(half * HALF + start), CHUNK), pl.ds(r * LANES, LANES)]

    coded(load(2, 0), far_a)
    coded(load(2, 1), far_b)
    coded(load(1, 1), after_b)
    coded(load(3, 0), before_a)
    after_a[...] = part[0:HALF, LANES : 2 * LANES]
    before_b[...] = part[HALF : 2 * HALF, 3 * LANES :]
    own[...] = part[0 : 2 * HALF, 0:LANES]


def products(mine, other, weights):
    code = jax.ShapeDtypeStruct((CODED, LANES), jnp.int32)
    half = jax.ShapeDtypeStruct((HALF, LANES), jnp.float32)
    return pl.pallas_call(
        product_kernel,
        out_shape=[code, code, code, code, half, half, jax.ShapeDtypeStruct((2 * HALF, LANES), jnp.float32)],
        in_specs=[WHOLE, WHOLE, pl.BlockSpec(memory_space=pltpu.HBM)],
        out_specs=[WHOLE] * 7,
        scratch_shapes=[
            pltpu.VMEM((ROWS, DEPTH), jnp.bfloat16),
            pltpu.VMEM((NX * LANES, DEPTH), jnp.bfloat16),
            pltpu.VMEM((2 * HALF, NX * LANES), jnp.float32),
            pltpu.SemaphoreType.DMA((len(BLOCKS),)),
        ],
        compiler_params=pltpu.CompilerParams(vmem_limit_bytes=44 << 20),
        cost_estimate=pl.CostEstimate(flops=2 * ROWS * 512 * DEPTH, bytes_accessed=ROWS * DEPTH * 2, transcendentals=0),
        name="products",
    )(mine, other, weights)


def relay_kernel(far_a, far_b, after_a, before_b, after_out, before_out, total):
    for far, own, out in ((far_a, after_a, after_out), (far_b, before_b, before_out)):
        step = step_of(far)

        def add(j, carry):
            for third, value in enumerate(decoded(far, step, j)):
                at = pl.ds(aligned(third * THIRD + j * CHUNK), CHUNK)
                total[at, :] = own[at, :] + value
            return carry

        lax.fori_loop(0, STEPS, add, 0)
        coded(lambda start: total[pl.ds(aligned(start), CHUNK), :], out)


def relayed(far_a, far_b, after_a, before_b):
    code = jax.ShapeDtypeStruct((CODED, LANES), jnp.int32)
    return pl.pallas_call(
        relay_kernel,
        out_shape=[code, code],
        in_specs=[WHOLE] * 4,
        out_specs=[WHOLE] * 2,
        scratch_shapes=[pltpu.VMEM((HALF, LANES), jnp.float32)],
        compiler_params=pltpu.CompilerParams(vmem_limit_bytes=16 << 20),
        cost_estimate=pl.CostEstimate(flops=20 * HALF * LANES, bytes_accessed=4 * HALF * LANES * 4, transcendentals=0),
        name="relayed",
    )(far_a, far_b, after_a, before_b)


def scores_kernel(
    own, a_one, a_two, b_one, b_two, context, emitted, fresh, divisor, fine, appearance, softness,
    scores, line, copies,
):
    factor = divisor[...]
    inverse = 1.0 / factor
    per_count = fine[...]
    per_word = appearance[...]
    cooling = 1.0 / softness[...]
    newest = fresh[...] - shard_index() * ROWS

    def chunk(j, carry, half, first, second, steps, sizes):
        pairs = zip(decoded(first, steps[0], j), decoded(second, steps[1], j))
        for third, (one, two) in enumerate(pairs):
            size = sizes[third]
            start = half * HALF + third * THIRD + j * CHUNK
            at = pl.ds(aligned(start), size)
            logits = own[at, :] + one[:size] + two[:size]
            ids = start + lax.broadcasted_iota(jnp.int32, (size, LANES), 0)
            counts = emitted[at, :] + (ids == newest).astype(jnp.int32)
            seen = context[at, :] + counts > 0
            moved_score = jnp.where(logits > 0, logits * inverse, logits * factor)
            score = jnp.where(seen, moved_score, logits)
            score = score - per_count * counts.astype(jnp.float32)
            score = score - jnp.where(counts > 0, per_word, 0.0)
            score = score * cooling
            scores[at, :] = score
            if size == CHUNK:
                score = jnp.max(score.reshape(CHUNK // 8, 8, LANES), axis=0)
            carry = jnp.maximum(carry, jnp.max(score, axis=0, keepdims=True) if size < CHUNK else score)
        return carry

    top = jnp.full((8, LANES), -jnp.inf, jnp.float32)
    for half, first, second in ((0, a_one, a_two), (1, b_one, b_two)):
        steps = (step_of(first), step_of(second))
        full = (CHUNK,) * 3

        def body(j, carry):
            return chunk(j, carry, half, first, second, steps, full)

        top = lax.fori_loop(0, STEPS - 1, body, top)
        last = CHUNK - half * (2 * HALF - ROWS)
        top = chunk(STEPS - 1, top, half, first, second, steps, (CHUNK, CHUNK, last))
    top = jnp.max(top, axis=0, keepdims=True)

    def run(j, total):
        value = jnp.exp(scores[pl.ds(aligned(j * 80), 80), :] - top)
        return total + jnp.sum(value.reshape(10, 8, LANES), axis=0)

    total = lax.fori_loop(0, 25, run, jnp.zeros((8, LANES), jnp.float32))
    total = jnp.sum(total, axis=0, keepdims=True)
    total = total + jnp.sum(jnp.exp(scores[2000:ROWS, :] - top), axis=0, keepdims=True)
    line[...] = top
    copies[:, 0:1, :] = jnp.broadcast_to(top[None], (64, 1, LANES))
    copies[:, 1:2, :] = jnp.broadcast_to(total[None], (64, 1, LANES))


def scored(*args):
    full = jax.ShapeDtypeStruct((ROWS, LANES), jnp.float32)
    line = jax.ShapeDtypeStruct((1, LANES), jnp.float32)
    return pl.pallas_call(
        scores_kernel,
        out_shape=[full, line, jax.ShapeDtypeStruct((64, 2, LANES), jnp.float32)],
        in_specs=[WHOLE] * 12,
        out_specs=[WHOLE] * 3,
        compiler_params=pltpu.CompilerParams(vmem_limit_bytes=24 << 20),
        cost_estimate=pl.CostEstimate(flops=30 * ROWS * LANES, bytes_accessed=6 * ROWS * LANES * 4, transcendentals=ROWS * LANES),
        name="scored",
    )(*args)


def prefix_kernel(scores, line, emitted, fresh, before, counts):
    newest = fresh[...] - shard_index() * ROWS
    ids = lax.broadcasted_iota(jnp.int32, (8, LANES), 0)
    top = line[...]

    def run(j, carry):
        for t in range(10):
            at = pl.ds(aligned(j * 80 + 8 * t), 8)
            value = jnp.exp(scores[at, :] - top)
            upto = value
            for shift in (1, 2, 4):
                upto = upto + jnp.where(ids >= shift, pltpu.roll(upto, shift, 0), 0.0)
            before[at, :] = (upto - value) + carry
            carry = carry + upto[7:8, :]
            counts[at, :] = emitted[at, :] + (ids + (j * 80 + 8 * t) == newest).astype(jnp.int32)
        return carry

    carry = lax.fori_loop(0, 25, run, jnp.zeros((1, LANES), jnp.float32))
    for row in range(2000, ROWS):
        before[row : row + 1, :] = carry
        carry = carry + jnp.exp(scores[row : row + 1, :] - top)
        counts[row : row + 1, :] = emitted[row : row + 1, :] + (newest == row).astype(jnp.int32)


def prefixes(scores, line, emitted, fresh):
    return pl.pallas_call(
        prefix_kernel,
        out_shape=[
            jax.ShapeDtypeStruct((ROWS, LANES), jnp.float32),
            jax.ShapeDtypeStruct((ROWS, LANES), jnp.int32),
        ],
        in_specs=[WHOLE] * 4,
        out_specs=[WHOLE] * 2,
        compiler_params=pltpu.CompilerParams(vmem_limit_bytes=8 << 20),
        cost_estimate=pl.CostEstimate(flops=400 * ROWS * LANES, bytes_accessed=2 * ROWS * LANES * 4, transcendentals=0),
        name="prefixes",
    )(scores, line, emitted, fresh)


def quantile_kernel(stats, line, draws, scores, before, copies, shift):
    shard = shard_index()
    top = jnp.max(stats[...], axis=0)[0:1, :]
    total = jnp.zeros((1, LANES), jnp.float32)
    lower = total
    for peer in range(64):
        part = stats[peer, 1:2, :] * jnp.exp(stats[peer, 0:1, :] - top)
        total = total + part
        lower = lower + jnp.where(peer < shard, part, 0.0)
    mine = line[...]
    share = jnp.exp(mine - top) / total
    room = draws[...] - lower / total
    first = shard * ROWS

    def taken(start, size):
        at = pl.ds(start, size)
        mass = jnp.exp(scores[at, :] - mine) * share
        value = jnp.minimum(jnp.maximum(room - before[at, :] * share, 0.0), mass)
        ids = first + start + lax.broadcasted_iota(jnp.int32, (size, LANES), 0)
        return value * ((ids.astype(jnp.float32) + 0.5) / VOCAB)

    def run(j, total):
        return total + jnp.sum(taken(aligned(j * 80), 80).reshape(10, 8, LANES), axis=0)

    amount = lax.fori_loop(0, 25, run, jnp.zeros((8, LANES), jnp.float32))
    amount = jnp.sum(amount, axis=0, keepdims=True) + jnp.sum(taken(2000, 4), axis=0, keepdims=True)
    copies[...] = jnp.broadcast_to(amount[None], (64, 1, LANES))
    shift[...] = top + jnp.log(total)


def quantiles(*args):
    return pl.pallas_call(
        quantile_kernel,
        out_shape=[
            jax.ShapeDtypeStruct((64, 1, LANES), jnp.float32),
            jax.ShapeDtypeStruct((1, LANES), jnp.float32),
        ],
        in_specs=[WHOLE] * 5,
        out_specs=[WHOLE] * 2,
        compiler_params=pltpu.CompilerParams(vmem_limit_bytes=8 << 20),
        cost_estimate=pl.CostEstimate(flops=10 * ROWS * LANES, bytes_accessed=2 * ROWS * LANES * 4, transcendentals=0),
        name="quantiles",
    )(*args)


def on_device(
    final_activation,
    output_projection_weights,
    context_word_tallies,
    emitted_word_tallies,
    freshest_word,
    recurrence_divisor,
    recurrence_fine,
    appearance_fine,
    softness_level,
    random_draws,
):
    fresh = freshest_word[None]
    emitted = emitted_word_tallies.T

    mine = moved(final_activation, lambda x, y, z, c: (y, x, z, c))
    mine = copies_from(mine, "z")
    mine = copies_from(mine, "y")
    other = moved(mine, lambda x, y, z, c: (x, y, z, 1 - c))
    far_a, far_b, after_b, before_a, after_a, before_b, own = products(
        mine, other, output_projection_weights.T
    )

    far_a, far_b = up(far_a), down(far_b)
    b_one, a_one = up(after_b), down(before_a)
    after_a, before_b = relayed(far_a, far_b, after_a, before_b)
    a_two, b_two = up(after_a), down(before_b)

    scores, local_top, copies = scored(
        own,
        a_one,
        a_two,
        b_one,
        b_two,
        context_word_tallies.T,
        emitted,
        fresh,
        recurrence_divisor[None],
        recurrence_fine[None],
        appearance_fine[None],
        softness_level[None],
    )

    stats = exchanged(copies)
    before, new_counts = prefixes(scores, local_top, emitted, fresh)
    copies, shift = quantiles(stats, local_top, random_draws[None], scores, before)
    sample_quantile = jnp.sum(exchanged(copies), axis=(0, 1))
    log_likelihoods = (scores - shift).T
    return new_counts.T, log_likelihoods, sample_quantile


def solution(mesh):
    split = Mesh(mesh.devices.reshape(NX, NY, NZ, NC), EVERY)
    whole = P("x", PLANE)
    row = P("x")
    return jax.shard_map(
        on_device,
        mesh=split,
        in_specs=(whole, whole, whole, whole, row, row, row, row, row, row),
        out_specs=(whole, whole, row),
        check_vma=False,
    )
```

```python
import jax
import jax.numpy as jnp
from jax import lax
from jax.experimental import pallas as pl
from jax.experimental.pallas import tpu as pltpu
from jax.sharding import Mesh
from jax.sharding import PartitionSpec as P


VOCAB = 128256
NX, NY, NZ, NC = 4, 4, 8, 2
PLANE = ("y", "z", "c")
EVERY = ("x", "y", "z", "c")

ROWS = 2004
LANES = 128
DEPTH = 2048
HALF = 1008
THIRD = HALF // 3
CHUNK = 56
STEPS = THIRD // CHUNK
BLOCKS = ((0, 512), (512, 512), (1024, 512), (1536, ROWS - 1536))
CODED = 2 * THIRD + 8
BITS = 20

WHOLE = pl.BlockSpec(memory_space=pltpu.VMEM)


def moved(value, to):
    pairs = []
    for x in range(NX):
        for y in range(NY):
            for z in range(NZ):
                for c in range(NC):
                    tx, ty, tz, tc = to(x, y, z, c)
                    source = ((x * NY + y) * NZ + z) * NC + c
                    target = ((tx % NX * NY + ty % NY) * NZ + tz % NZ) * NC + tc % NC
                    pairs.append((source, target))
    return lax.ppermute(value, EVERY, pairs)


def up(value):
    return moved(value, lambda x, y, z, c: (x + 1, y, z, c))


def down(value):
    return moved(value, lambda x, y, z, c: (x - 1, y, z, c))


def copies_from(value, axis):
    size = lax.axis_size(axis)
    copies = jnp.broadcast_to(value, (size, *value.shape))
    return lax.all_to_all(copies, axis, split_axis=0, concat_axis=0, tiled=True)


def exchanged(copies):
    return lax.all_to_all(copies, PLANE, split_axis=0, concat_axis=0, tiled=True)


def coded(load, out_ref):
    def largest(j, top):
        for third in range(3):
            part = jnp.abs(load(third * THIRD + j * CHUNK))
            top = jnp.maximum(top, jnp.max(part.reshape(CHUNK // 8, 8, LANES), axis=0))
        return top

    top = lax.fori_loop(0, STEPS, largest, jnp.zeros((8, LANES), jnp.float32))
    top = jnp.maximum(jnp.max(top, axis=0, keepdims=True), 1e-30)
    exponent = jnp.ceil(4.0 * jnp.log2(top))
    scale = jnp.exp2(BITS - 0.25 * exponent)
    limit = float(2**BITS - 1)

    def put(j, carry):
        def whole(third):
            value = jnp.round(load(third * THIRD + j * CHUNK) * scale)
            return jnp.clip(value, -limit, limit).astype(jnp.int32)

        a, b, c = whole(0), whole(1), whole(2)
        mask = (1 << 21) - 1
        out_ref[pl.ds(pl.multiple_of(j * CHUNK, 8), CHUNK), :] = (a & mask) | (c << 21)
        out_ref[pl.ds(pl.multiple_of(THIRD + j * CHUNK, 8), CHUNK), :] = (b & mask) | ((c >> 11) << 21)
        return carry

    lax.fori_loop(0, STEPS, put, 0)
    out_ref[2 * THIRD :, :] = jnp.broadcast_to(exponent.astype(jnp.int32), (8, LANES))


def step_of(ref):
    return jnp.exp2(0.25 * ref[2 * THIRD : 2 * THIRD + 1, :].astype(jnp.float32) - BITS)


def decoded(ref, step, j):
    one = ref[pl.ds(pl.multiple_of(j * CHUNK, 8), CHUNK), :]
    two = ref[pl.ds(pl.multiple_of(THIRD + j * CHUNK, 8), CHUNK), :]
    a = (one << 11) >> 11
    b = (two << 11) >> 11
    c = ((two >> 21) << 11) | ((one >> 21) & 2047)
    return [value.astype(jnp.float32) * step for value in (a, b, c)]


def aligned(start):
    return pl.multiple_of(start, 8)


def shard_index():
    return (lax.axis_index("y") * NZ + lax.axis_index("z")) * NC + lax.axis_index("c")


def slot_of(r):
    return lax.rem(lax.axis_index("x") + r + NY - lax.axis_index("y"), NY)


def fetch_kernel(source, out, here):
    copies = [
        pltpu.make_async_copy(source.at[pl.ds(start, size)], out.at[pl.ds(start, size)], here.at[n])
        for n, (start, size) in enumerate(BLOCKS)
    ]
    for copy in copies:
        copy.start()
    for copy in copies:
        copy.wait()


def fetched(weights):
    return pl.pallas_call(
        fetch_kernel,
        out_shape=jax.ShapeDtypeStruct(weights.shape, weights.dtype),
        in_specs=[pl.BlockSpec(memory_space=pltpu.HBM)],
        out_specs=WHOLE,
        scratch_shapes=[pltpu.SemaphoreType.DMA((len(BLOCKS),))],
        compiler_params=pltpu.CompilerParams(vmem_limit_bytes=44 << 20),
        cost_estimate=pl.CostEstimate(flops=ROWS * DEPTH * 512, bytes_accessed=ROWS * DEPTH * 4, transcendentals=0),
        name="fetched",
    )(weights)


def lay_out(rows, row, block, core):
    for z in range(NZ):
        at = pl.ds(pl.multiple_of((2 * z + core) * 128, 128), 128)
        rows[pl.ds(pl.multiple_of(row, 128), LANES), at] = block[z]


def multiplied(weights, rows, put):
    for start, size in BLOCKS:
        put(
            start,
            size,
            lax.dot_general(
                weights[pl.ds(start, size), :],
                rows[...],
                (((1,), (1,)), ((), ())),
                preferred_element_type=jnp.float32,
            ),
        )


def clear_tail(parts, slot):
    parts[slot, ROWS : 2 * HALF, :] = jnp.zeros((2 * HALF - ROWS, LANES), jnp.float32)


def first_kernel(mine, other, weights, parts, rows):
    c = lax.axis_index("c")
    lay_out(rows, 0, mine, c)
    lay_out(rows, 0, other, 1 - c)

    def put(start, size, value):
        parts[0, pl.ds(start, size), :] = value

    multiplied(weights, rows, put)
    clear_tail(parts, 0)


def second_kernel(one, two, other_one, other_two, weights, given, parts, rows):
    c = lax.axis_index("c")
    lay_out(rows, c * LANES, one, c)
    lay_out(rows, (1 - c) * LANES, two, c)
    lay_out(rows, (1 - c) * LANES, other_one, 1 - c)
    lay_out(rows, c * LANES, other_two, 1 - c)

    def put(start, size, value):
        parts[3, pl.ds(start, size), :] = value[:, :LANES]
        parts[1, pl.ds(start, size), :] = value[:, LANES:]

    multiplied(weights, rows, put)
    clear_tail(parts, 3)
    clear_tail(parts, 1)


def part_of(parts, r, half):
    slot = slot_of(r)
    return lambda start: parts[slot, pl.ds(aligned(half * HALF + start), CHUNK), :]


def third_kernel(mine, other, weights, given, parts, far_a, far_b, rows):
    c = lax.axis_index("c")
    lay_out(rows, 0, mine, c)
    lay_out(rows, 0, other, 1 - c)

    def put(start, size, value):
        parts[2, pl.ds(start, size), :] = value

    multiplied(weights, rows, put)
    clear_tail(parts, 2)
    coded(part_of(parts, 2, 0), far_a)
    coded(part_of(parts, 2, 1), far_b)


def near_kernel(parts, after_b, before_a):
    coded(part_of(parts, 1, 1), after_b)
    coded(part_of(parts, 3, 0), before_a)


PARTS = jax.ShapeDtypeStruct((NY, 2 * HALF, LANES), jnp.float32)
CODE = jax.ShapeDtypeStruct((CODED, LANES), jnp.int32)


def multiply(kernel, groups, extra, *args):
    given = len(args) - 1 if kernel is not first_kernel else None
    return pl.pallas_call(
        kernel,
        out_shape=[PARTS] + extra,
        in_specs=[WHOLE] * len(args),
        out_specs=[WHOLE] * (1 + len(extra)),
        scratch_shapes=[pltpu.VMEM((groups * LANES, DEPTH), jnp.bfloat16)],
        input_output_aliases={} if given is None else {given: 0},
        compiler_params=pltpu.CompilerParams(vmem_limit_bytes=12 << 20),
        cost_estimate=pl.CostEstimate(
            flops=2 * ROWS * 256 * DEPTH, bytes_accessed=ROWS * DEPTH * 2, transcendentals=0
        ),
    )(*args)


def near(parts):
    return pl.pallas_call(
        near_kernel,
        out_shape=[CODE, CODE],
        in_specs=[WHOLE],
        out_specs=[WHOLE] * 2,
        compiler_params=pltpu.CompilerParams(vmem_limit_bytes=8 << 20),
        cost_estimate=pl.CostEstimate(flops=20 * HALF * LANES, bytes_accessed=4 * HALF * LANES * 4, transcendentals=0),
        name="near",
    )(parts)


def relay_kernel(far_a, far_b, parts, after_out, before_out, total):
    for r, half, far, out in ((1, 0, far_a, after_out), (3, 1, far_b, before_out)):
        step = step_of(far)
        own = part_of(parts, r, half)

        def add(j, carry):
            for third, value in enumerate(decoded(far, step, j)):
                start = third * THIRD + j * CHUNK
                total[pl.ds(aligned(start), CHUNK), :] = own(start) + value
            return carry

        lax.fori_loop(0, STEPS, add, 0)
        coded(lambda start: total[pl.ds(aligned(start), CHUNK), :], out)


def relayed(far_a, far_b, parts):
    return pl.pallas_call(
        relay_kernel,
        out_shape=[CODE, CODE],
        in_specs=[WHOLE] * 3,
        out_specs=[WHOLE] * 2,
        scratch_shapes=[pltpu.VMEM((HALF, LANES), jnp.float32)],
        compiler_params=pltpu.CompilerParams(vmem_limit_bytes=8 << 20),
        cost_estimate=pl.CostEstimate(flops=20 * HALF * LANES, bytes_accessed=4 * HALF * LANES * 4, transcendentals=0),
        name="relayed",
    )(far_a, far_b, parts)


def scores_kernel(
    parts, a_one, a_two, b_one, b_two, context, emitted, fresh, divisor, fine, appearance, softness,
    scores, line, copies,
):
    slot = slot_of(0)
    factor = divisor[...]
    inverse = 1.0 / factor
    per_count = fine[...]
    per_word = appearance[...]
    cooling = 1.0 / softness[...]
    newest = fresh[...] - shard_index() * ROWS

    def chunk(j, carry, half, first, second, steps, sizes):
        pairs = zip(decoded(first, steps[0], j), decoded(second, steps[1], j))
        for third, (one, two) in enumerate(pairs):
            size = sizes[third]
            start = half * HALF + third * THIRD + j * CHUNK
            at = pl.ds(aligned(start), size)
            logits = parts[slot, at, :] + one[:size] + two[:size]
            ids = start + lax.broadcasted_iota(jnp.int32, (size, LANES), 0)
            counts = emitted[at, :] + (ids == newest).astype(jnp.int32)
            seen = context[at, :] + counts > 0
            moved_score = jnp.where(logits > 0, logits * inverse, logits * factor)
            score = jnp.where(seen, moved_score, logits)
            score = score - per_count * counts.astype(jnp.float32)
            score = score - jnp.where(counts > 0, per_word, 0.0)
            score = score * cooling
            scores[at, :] = score
            if size == CHUNK:
                score = jnp.max(score.reshape(CHUNK // 8, 8, LANES), axis=0)
            carry = jnp.maximum(carry, jnp.max(score, axis=0, keepdims=True) if size < CHUNK else score)
        return carry

    top = jnp.full((8, LANES), -jnp.inf, jnp.float32)
    for half, first, second in ((0, a_one, a_two), (1, b_one, b_two)):
        steps = (step_of(first), step_of(second))
        full = (CHUNK,) * 3

        def body(j, carry):
            return chunk(j, carry, half, first, second, steps, full)

        top = lax.fori_loop(0, STEPS - 1, body, top)
        last = CHUNK - half * (2 * HALF - ROWS)
        top = chunk(STEPS - 1, top, half, first, second, steps, (CHUNK, CHUNK, last))
    top = jnp.max(top, axis=0, keepdims=True)

    def run(j, total):
        value = jnp.exp(scores[pl.ds(aligned(j * 80), 80), :] - top)
        return total + jnp.sum(value.reshape(10, 8, LANES), axis=0)

    total = lax.fori_loop(0, 25, run, jnp.zeros((8, LANES), jnp.float32))
    total = jnp.sum(total, axis=0, keepdims=True)
    total = total + jnp.sum(jnp.exp(scores[2000:ROWS, :] - top), axis=0, keepdims=True)
    line[...] = top
    copies[:, 0:1, :] = jnp.broadcast_to(top[None], (64, 1, LANES))
    copies[:, 1:2, :] = jnp.broadcast_to(total[None], (64, 1, LANES))


def scored(*args):
    full = jax.ShapeDtypeStruct((ROWS, LANES), jnp.float32)
    line = jax.ShapeDtypeStruct((1, LANES), jnp.float32)
    return pl.pallas_call(
        scores_kernel,
        out_shape=[full, line, jax.ShapeDtypeStruct((64, 2, LANES), jnp.float32)],
        in_specs=[WHOLE] * 12,
        out_specs=[WHOLE] * 3,
        compiler_params=pltpu.CompilerParams(vmem_limit_bytes=24 << 20),
        cost_estimate=pl.CostEstimate(flops=30 * ROWS * LANES, bytes_accessed=6 * ROWS * LANES * 4, transcendentals=ROWS * LANES),
        name="scored",
    )(*args)


def prefix_kernel(scores, line, emitted, fresh, before, counts):
    newest = fresh[...] - shard_index() * ROWS
    ids = lax.broadcasted_iota(jnp.int32, (8, LANES), 0)
    top = line[...]

    def run(j, carry):
        for t in range(10):
            at = pl.ds(aligned(j * 80 + 8 * t), 8)
            value = jnp.exp(scores[at, :] - top)
            upto = value
            for shift in (1, 2, 4):
                upto = upto + jnp.where(ids >= shift, pltpu.roll(upto, shift, 0), 0.0)
            before[at, :] = (upto - value) + carry
            carry = carry + upto[7:8, :]
            counts[at, :] = emitted[at, :] + (ids + (j * 80 + 8 * t) == newest).astype(jnp.int32)
        return carry

    carry = lax.fori_loop(0, 25, run, jnp.zeros((1, LANES), jnp.float32))
    for row in range(2000, ROWS):
        before[row : row + 1, :] = carry
        carry = carry + jnp.exp(scores[row : row + 1, :] - top)
        counts[row : row + 1, :] = emitted[row : row + 1, :] + (newest == row).astype(jnp.int32)


def prefixes(scores, line, emitted, fresh):
    return pl.pallas_call(
        prefix_kernel,
        out_shape=[
            jax.ShapeDtypeStruct((ROWS, LANES), jnp.float32),
            jax.ShapeDtypeStruct((ROWS, LANES), jnp.int32),
        ],
        in_specs=[WHOLE] * 4,
        out_specs=[WHOLE] * 2,
        compiler_params=pltpu.CompilerParams(vmem_limit_bytes=8 << 20),
        cost_estimate=pl.CostEstimate(flops=400 * ROWS * LANES, bytes_accessed=2 * ROWS * LANES * 4, transcendentals=0),
        name="prefixes",
    )(scores, line, emitted, fresh)


def quantile_kernel(stats, line, draws, scores, before, copies, shift):
    shard = shard_index()
    top = jnp.max(stats[...], axis=0)[0:1, :]
    total = jnp.zeros((1, LANES), jnp.float32)
    lower = total
    for peer in range(64):
        part = stats[peer, 1:2, :] * jnp.exp(stats[peer, 0:1, :] - top)
        total = total + part
        lower = lower + jnp.where(peer < shard, part, 0.0)
    mine = line[...]
    share = jnp.exp(mine - top) / total
    room = draws[...] - lower / total
    first = shard * ROWS

    def taken(start, size):
        at = pl.ds(start, size)
        mass = jnp.exp(scores[at, :] - mine) * share
        value = jnp.minimum(jnp.maximum(room - before[at, :] * share, 0.0), mass)
        ids = first + start + lax.broadcasted_iota(jnp.int32, (size, LANES), 0)
        return value * ((ids.astype(jnp.float32) + 0.5) / VOCAB)

    def run(j, total):
        return total + jnp.sum(taken(aligned(j * 80), 80).reshape(10, 8, LANES), axis=0)

    amount = lax.fori_loop(0, 25, run, jnp.zeros((8, LANES), jnp.float32))
    amount = jnp.sum(amount, axis=0, keepdims=True) + jnp.sum(taken(2000, 4), axis=0, keepdims=True)
    copies[...] = jnp.broadcast_to(amount[None], (64, 1, LANES))
    shift[...] = top + jnp.log(total)


def quantiles(*args):
    return pl.pallas_call(
        quantile_kernel,
        out_shape=[
            jax.ShapeDtypeStruct((64, 1, LANES), jnp.float32),
            jax.ShapeDtypeStruct((1, LANES), jnp.float32),
        ],
        in_specs=[WHOLE] * 5,
        out_specs=[WHOLE] * 2,
        compiler_params=pltpu.CompilerParams(vmem_limit_bytes=8 << 20),
        cost_estimate=pl.CostEstimate(flops=10 * ROWS * LANES, bytes_accessed=2 * ROWS * LANES * 4, transcendentals=0),
        name="quantiles",
    )(*args)


def step(
    final_activation,
    output_projection_weights,
    context_word_tallies,
    emitted_word_tallies,
    freshest_word,
    recurrence_divisor,
    recurrence_fine,
    appearance_fine,
    softness_level,
    random_draws,
):
    fresh = freshest_word[None]
    emitted = emitted_word_tallies.T

    mine = moved(final_activation, lambda x, y, z, c: (y, x, z, c))
    mine = copies_from(mine, "z")

    def partner(value):
        return moved(value, lambda x, y, z, c: (x, y, z, 1 - c))

    def onward(value):
        return moved(value, lambda x, y, z, c: (x, y + 1 - 2 * c, z, c))

    def backward(value):
        return moved(value, lambda x, y, z, c: (x, y - 1 + 2 * c, z, c))

    other = partner(mine)
    one = onward(mine)
    two = backward(mine)
    weights = fetched(output_projection_weights.T)
    last = onward(one)
    other_one = partner(one)
    other_two = partner(two)
    (parts,) = multiply(first_kernel, 1, [], mine, other, weights)
    (parts,) = multiply(second_kernel, 2, [], one, two, other_one, other_two, weights, parts)
    other_last = partner(last)
    parts, far_a, far_b = multiply(third_kernel, 1, [CODE, CODE], last, other_last, weights, parts)

    far_a = up(far_a)
    far_b = down(far_b)
    after_b, before_a = near(parts)
    b_one, a_one = up(after_b), down(before_a)
    after_a, before_b = relayed(far_a, far_b, parts)
    a_two, b_two = up(after_a), down(before_b)

    scores, local_top, copies = scored(
        parts,
        a_one,
        a_two,
        b_one,
        b_two,
        context_word_tallies.T,
        emitted,
        fresh,
        recurrence_divisor[None],
        recurrence_fine[None],
        appearance_fine[None],
        softness_level[None],
    )

    stats = exchanged(copies)
    before, new_counts = prefixes(scores, local_top, emitted, fresh)
    copies, shift = quantiles(stats, local_top, random_draws[None], scores, before)
    sample_quantile = jnp.sum(exchanged(copies), axis=(0, 1))
    log_likelihoods = (scores - shift).T
    return new_counts.T, log_likelihoods, sample_quantile


def solution(mesh):
    split = Mesh(mesh.devices.reshape(NX, NY, NZ, NC), EVERY)
    whole = P("x", PLANE)
    row = P("x")
    return jax.shard_map(
        step,
        mesh=split,
        in_specs=(whole, whole, whole, whole, row, row, row, row, row, row),
        out_specs=(whole, whole, row),
        check_vma=False,
    )
```

```python
import jax
import jax.numpy as jnp
from jax import lax
from jax.experimental import pallas as pl
from jax.experimental.pallas import tpu as pltpu
from jax.sharding import Mesh
from jax.sharding import PartitionSpec as P


VOCAB = 128256
NX, NY, NZ, NC = 4, 4, 8, 2
PLANE = ("y", "z", "c")
EVERY = ("x", "y", "z", "c")

ROWS = 2004
LANES = 128
DEPTH = 2048
HALF = 1008
PIECE = HALF // 7
CHUNK = 48
STEPS = PIECE // CHUNK
BLOCKS = ((0, 512), (512, 512), (1024, 512), (1536, ROWS - 1536))
CODED = 4 * PIECE + 8
BITS = 17

WHOLE = pl.BlockSpec(memory_space=pltpu.VMEM)


def moved(value, to):
    pairs = []
    for x in range(NX):
        for y in range(NY):
            for z in range(NZ):
                for c in range(NC):
                    tx, ty, tz, tc = to(x, y, z, c)
                    source = ((x * NY + y) * NZ + z) * NC + c
                    target = ((tx % NX * NY + ty % NY) * NZ + tz % NZ) * NC + tc % NC
                    pairs.append((source, target))
    return lax.ppermute(value, EVERY, pairs)


def up(value):
    return moved(value, lambda x, y, z, c: (x + 1, y, z, c))


def down(value):
    return moved(value, lambda x, y, z, c: (x - 1, y, z, c))


def copies_from(value, axis):
    size = lax.axis_size(axis)
    copies = jnp.broadcast_to(value, (size, *value.shape))
    return lax.all_to_all(copies, axis, split_axis=0, concat_axis=0, tiled=True)


def exchanged(copies):
    return lax.all_to_all(copies, PLANE, split_axis=0, concat_axis=0, tiled=True)


def coded(load, out_ref):
    def largest(j, top):
        for piece in range(7):
            part = jnp.abs(load(piece * PIECE + j * CHUNK))
            top = jnp.maximum(top, jnp.max(part.reshape(CHUNK // 8, 8, LANES), axis=0))
        return top

    top = lax.fori_loop(0, STEPS, largest, jnp.zeros((8, LANES), jnp.float32))
    top = jnp.maximum(jnp.max(top, axis=0, keepdims=True), 1e-30)
    exponent = jnp.ceil(4.0 * jnp.log2(top))
    scale = jnp.exp2(BITS - 0.25 * exponent)
    limit = float(2**BITS - 1)

    def put(j, carry):
        def whole(piece):
            value = jnp.round(load(piece * PIECE + j * CHUNK) * scale)
            return jnp.clip(value, -limit, limit).astype(jnp.int32)

        low = (1 << 18) - 1
        last = whole(3) & low
        for word in range(3):
            high = whole(4 + word)
            out_ref[pl.ds(aligned(word * PIECE + j * CHUNK), CHUNK), :] = (whole(word) & low) | (high << 18)
            last = last | (((high >> 14) & 15) << (18 + 4 * word))
        out_ref[pl.ds(aligned(3 * PIECE + j * CHUNK), CHUNK), :] = last
        return carry

    lax.fori_loop(0, STEPS, put, 0)
    out_ref[4 * PIECE :, :] = jnp.broadcast_to(exponent.astype(jnp.int32), (8, LANES))


def step_of(ref):
    return jnp.exp2(0.25 * ref[4 * PIECE : 4 * PIECE + 1, :].astype(jnp.float32) - BITS)


def decoded(ref, step, j):
    words = [ref[pl.ds(aligned(word * PIECE + j * CHUNK), CHUNK), :] for word in range(4)]
    values = [(word << 14) >> 14 for word in words]
    for n in range(3):
        high = (words[3] << (10 - 4 * n)) >> 28
        values.append((high << 14) | ((words[n] >> 18) & 0x3FFF))
    return [value.astype(jnp.float32) * step for value in values]


def aligned(start):
    return pl.multiple_of(start, 8)


def shard_index():
    return (lax.axis_index("y") * NZ + lax.axis_index("z")) * NC + lax.axis_index("c")


def slot_of(r):
    return lax.rem(lax.axis_index("x") + r + NY - lax.axis_index("y"), NY)


def fetch_kernel(source, out, here):
    copies = [
        pltpu.make_async_copy(source.at[pl.ds(start, size)], out.at[pl.ds(start, size)], here.at[n])
        for n, (start, size) in enumerate(BLOCKS)
    ]
    for copy in copies:
        copy.start()
    for copy in copies:
        copy.wait()


def fetched(weights):
    return pl.pallas_call(
        fetch_kernel,
        out_shape=jax.ShapeDtypeStruct(weights.shape, weights.dtype),
        in_specs=[pl.BlockSpec(memory_space=pltpu.HBM)],
        out_specs=WHOLE,
        scratch_shapes=[pltpu.SemaphoreType.DMA((len(BLOCKS),))],
        compiler_params=pltpu.CompilerParams(vmem_limit_bytes=44 << 20),
        cost_estimate=pl.CostEstimate(flops=ROWS * DEPTH * 512, bytes_accessed=ROWS * DEPTH * 4, transcendentals=0),
        name="fetched",
    )(weights)


def lay_out(rows, row, block, core):
    for z in range(NZ):
        at = pl.ds(pl.multiple_of((2 * z + core) * 128, 128), 128)
        rows[pl.ds(pl.multiple_of(row, 128), LANES), at] = block[z]


def multiplied(weights, rows, put):
    for start, size in BLOCKS:
        put(
            start,
            size,
            lax.dot_general(
                weights[pl.ds(start, size), :],
                rows[...],
                (((1,), (1,)), ((), ())),
                preferred_element_type=jnp.float32,
            ),
        )


def clear_tail(parts, slot):
    parts[slot, ROWS : 2 * HALF, :] = jnp.zeros((2 * HALF - ROWS, LANES), jnp.float32)


def first_kernel(mine, other, weights, parts, rows):
    c = lax.axis_index("c")
    lay_out(rows, 0, mine, c)
    lay_out(rows, 0, other, 1 - c)

    def put(start, size, value):
        parts[0, pl.ds(start, size), :] = value

    multiplied(weights, rows, put)
    clear_tail(parts, 0)


def second_kernel(one, two, other_one, other_two, weights, given, parts, rows):
    c = lax.axis_index("c")
    lay_out(rows, c * LANES, one, c)
    lay_out(rows, (1 - c) * LANES, two, c)
    lay_out(rows, (1 - c) * LANES, other_one, 1 - c)
    lay_out(rows, c * LANES, other_two, 1 - c)

    def put(start, size, value):
        parts[3, pl.ds(start, size), :] = value[:, :LANES]
        parts[1, pl.ds(start, size), :] = value[:, LANES:]

    multiplied(weights, rows, put)
    clear_tail(parts, 3)
    clear_tail(parts, 1)


def part_of(parts, r, half):
    slot = slot_of(r)
    return lambda start: parts[slot, pl.ds(aligned(half * HALF + start), CHUNK), :]


def third_kernel(mine, other, weights, given, parts, far_a, far_b, rows):
    c = lax.axis_index("c")
    lay_out(rows, 0, mine, c)
    lay_out(rows, 0, other, 1 - c)

    def put(start, size, value):
        parts[2, pl.ds(start, size), :] = value

    multiplied(weights, rows, put)
    clear_tail(parts, 2)
    coded(part_of(parts, 2, 0), far_a)
    coded(part_of(parts, 2, 1), far_b)


def near_kernel(parts, after_b, before_a):
    coded(part_of(parts, 1, 1), after_b)
    coded(part_of(parts, 3, 0), before_a)


PARTS = jax.ShapeDtypeStruct((NY, 2 * HALF, LANES), jnp.float32)
CODE = jax.ShapeDtypeStruct((CODED, LANES), jnp.int32)


def multiply(kernel, groups, extra, *args):
    given = len(args) - 1 if kernel is not first_kernel else None
    return pl.pallas_call(
        kernel,
        out_shape=[PARTS] + extra,
        in_specs=[WHOLE] * len(args),
        out_specs=[WHOLE] * (1 + len(extra)),
        scratch_shapes=[pltpu.VMEM((groups * LANES, DEPTH), jnp.bfloat16)],
        input_output_aliases={} if given is None else {given: 0},
        compiler_params=pltpu.CompilerParams(vmem_limit_bytes=12 << 20),
        cost_estimate=pl.CostEstimate(
            flops=2 * ROWS * 256 * DEPTH, bytes_accessed=ROWS * DEPTH * 2, transcendentals=0
        ),
    )(*args)


def near(parts):
    return pl.pallas_call(
        near_kernel,
        out_shape=[CODE, CODE],
        in_specs=[WHOLE],
        out_specs=[WHOLE] * 2,
        compiler_params=pltpu.CompilerParams(vmem_limit_bytes=8 << 20),
        cost_estimate=pl.CostEstimate(flops=20 * HALF * LANES, bytes_accessed=4 * HALF * LANES * 4, transcendentals=0),
        name="near",
    )(parts)


def relay_kernel(far_a, far_b, parts, after_out, before_out, total):
    for r, half, far, out in ((1, 0, far_a, after_out), (3, 1, far_b, before_out)):
        step = step_of(far)
        own = part_of(parts, r, half)

        def add(j, carry):
            for piece, value in enumerate(decoded(far, step, j)):
                start = piece * PIECE + j * CHUNK
                total[pl.ds(aligned(start), CHUNK), :] = own(start) + value
            return carry

        lax.fori_loop(0, STEPS, add, 0)
        coded(lambda start: total[pl.ds(aligned(start), CHUNK), :], out)


def relayed(far_a, far_b, parts):
    return pl.pallas_call(
        relay_kernel,
        out_shape=[CODE, CODE],
        in_specs=[WHOLE] * 3,
        out_specs=[WHOLE] * 2,
        scratch_shapes=[pltpu.VMEM((HALF, LANES), jnp.float32)],
        compiler_params=pltpu.CompilerParams(vmem_limit_bytes=8 << 20),
        cost_estimate=pl.CostEstimate(flops=20 * HALF * LANES, bytes_accessed=4 * HALF * LANES * 4, transcendentals=0),
        name="relayed",
    )(far_a, far_b, parts)


def chunks(half):
    full = [(piece, CHUNK) for piece in range(7)]
    last = full[:-1] + [(6, CHUNK - half * (2 * HALF - ROWS))]
    return full, last


def each_chunk(half, body, carry):
    full, last = chunks(half)

    def run(j, carry):
        return body(j, carry, full)

    carry = lax.fori_loop(0, STEPS - 1, run, carry)
    return body(STEPS - 1, carry, last)


def early_kernel(
    parts, a_one, b_one, context, emitted, fresh, divisor, fine, appearance, softness, sums, rising, falling, fines
):
    slot = slot_of(0)
    cooling = 1.0 / softness[...]
    seen_up = cooling / divisor[...]
    seen_down = cooling * divisor[...]
    per_count = fine[...] * cooling
    per_word = appearance[...] * cooling
    newest = fresh[...] - shard_index() * ROWS

    for half, one in ((0, a_one), (1, b_one)):
        step = step_of(one)

        def body(j, carry, pieces):
            for (piece, size), value in zip(pieces, decoded(one, step, j)):
                start = half * HALF + piece * PIECE + j * CHUNK
                at = pl.ds(aligned(start), size)
                sums[at, :] = parts[slot, at, :] + value[:size]
                ids = start + lax.broadcasted_iota(jnp.int32, (size, LANES), 0)
                counts = emitted[at, :] + (ids == newest).astype(jnp.int32)
                seen = context[at, :] + counts > 0
                rising[at, :] = jnp.where(seen, seen_up, cooling)
                falling[at, :] = jnp.where(seen, seen_down, cooling)
                fines[at, :] = per_count * counts.astype(jnp.float32) + jnp.where(counts > 0, per_word, 0.0)
            return carry

        each_chunk(half, body, 0)


def early(*args):
    full = jax.ShapeDtypeStruct((ROWS, LANES), jnp.float32)
    return pl.pallas_call(
        early_kernel,
        out_shape=[full] * 4,
        in_specs=[WHOLE] * 10,
        out_specs=[WHOLE] * 4,
        compiler_params=pltpu.CompilerParams(vmem_limit_bytes=8 << 20),
        cost_estimate=pl.CostEstimate(flops=30 * ROWS * LANES, bytes_accessed=9 * ROWS * LANES * 4, transcendentals=0),
        name="early",
    )(*args)


def scores_kernel(sums, rising, falling, fines, a_two, b_two, scores, line, copies):
    top = jnp.full((8, LANES), -jnp.inf, jnp.float32)
    for half, two in ((0, a_two), (1, b_two)):
        step = step_of(two)

        def body(j, carry, pieces):
            for (piece, size), value in zip(pieces, decoded(two, step, j)):
                at = pl.ds(aligned(half * HALF + piece * PIECE + j * CHUNK), size)
                logits = sums[at, :] + value[:size]
                score = logits * jnp.where(logits > 0, rising[at, :], falling[at, :]) - fines[at, :]
                scores[at, :] = score
                if size == CHUNK:
                    score = jnp.max(score.reshape(CHUNK // 8, 8, LANES), axis=0)
                else:
                    score = jnp.max(score, axis=0, keepdims=True)
                carry = jnp.maximum(carry, score)
            return carry

        top = each_chunk(half, body, top)
    top = jnp.max(top, axis=0, keepdims=True)

    def run(j, total):
        value = jnp.exp(scores[pl.ds(aligned(j * 80), 80), :] - top)
        return total + jnp.sum(value.reshape(10, 8, LANES), axis=0)

    total = lax.fori_loop(0, 25, run, jnp.zeros((8, LANES), jnp.float32))
    total = jnp.sum(total, axis=0, keepdims=True)
    total = total + jnp.sum(jnp.exp(scores[2000:ROWS, :] - top), axis=0, keepdims=True)
    line[...] = top
    copies[:, 0:1, :] = jnp.broadcast_to(top[None], (64, 1, LANES))
    copies[:, 1:2, :] = jnp.broadcast_to(total[None], (64, 1, LANES))


def scored(*args):
    full = jax.ShapeDtypeStruct((ROWS, LANES), jnp.float32)
    line = jax.ShapeDtypeStruct((1, LANES), jnp.float32)
    return pl.pallas_call(
        scores_kernel,
        out_shape=[full, line, jax.ShapeDtypeStruct((64, 2, LANES), jnp.float32)],
        in_specs=[WHOLE] * 6,
        out_specs=[WHOLE] * 3,
        compiler_params=pltpu.CompilerParams(vmem_limit_bytes=8 << 20),
        cost_estimate=pl.CostEstimate(flops=30 * ROWS * LANES, bytes_accessed=6 * ROWS * LANES * 4, transcendentals=ROWS * LANES),
        name="scored",
    )(*args)


def prefix_kernel(scores, line, emitted, fresh, before, counts):
    newest = fresh[...] - shard_index() * ROWS
    ids = lax.broadcasted_iota(jnp.int32, (8, LANES), 0)
    top = line[...]

    def run(j, carry):
        for t in range(10):
            at = pl.ds(aligned(j * 80 + 8 * t), 8)
            value = jnp.exp(scores[at, :] - top)
            upto = value
            for shift in (1, 2, 4):
                upto = upto + jnp.where(ids >= shift, pltpu.roll(upto, shift, 0), 0.0)
            before[at, :] = (upto - value) + carry
            carry = carry + upto[7:8, :]
            counts[at, :] = emitted[at, :] + (ids + (j * 80 + 8 * t) == newest).astype(jnp.int32)
        return carry

    carry = lax.fori_loop(0, 25, run, jnp.zeros((1, LANES), jnp.float32))
    for row in range(2000, ROWS):
        before[row : row + 1, :] = carry
        carry = carry + jnp.exp(scores[row : row + 1, :] - top)
        counts[row : row + 1, :] = emitted[row : row + 1, :] + (newest == row).astype(jnp.int32)


def prefixes(scores, line, emitted, fresh):
    return pl.pallas_call(
        prefix_kernel,
        out_shape=[
            jax.ShapeDtypeStruct((ROWS, LANES), jnp.float32),
            jax.ShapeDtypeStruct((ROWS, LANES), jnp.int32),
        ],
        in_specs=[WHOLE] * 4,
        out_specs=[WHOLE] * 2,
        compiler_params=pltpu.CompilerParams(vmem_limit_bytes=8 << 20),
        cost_estimate=pl.CostEstimate(flops=400 * ROWS * LANES, bytes_accessed=2 * ROWS * LANES * 4, transcendentals=0),
        name="prefixes",
    )(scores, line, emitted, fresh)


def quantile_kernel(stats, line, draws, scores, before, copies, shift):
    shard = shard_index()
    top = jnp.max(stats[...], axis=0)[0:1, :]
    total = jnp.zeros((1, LANES), jnp.float32)
    lower = total
    for peer in range(64):
        part = stats[peer, 1:2, :] * jnp.exp(stats[peer, 0:1, :] - top)
        total = total + part
        lower = lower + jnp.where(peer < shard, part, 0.0)
    mine = line[...]
    share = jnp.exp(mine - top) / total
    room = draws[...] - lower / total
    first = shard * ROWS

    def taken(start, size):
        at = pl.ds(start, size)
        mass = jnp.exp(scores[at, :] - mine) * share
        value = jnp.minimum(jnp.maximum(room - before[at, :] * share, 0.0), mass)
        ids = first + start + lax.broadcasted_iota(jnp.int32, (size, LANES), 0)
        return value * ((ids.astype(jnp.float32) + 0.5) / VOCAB)

    def run(j, total):
        return total + jnp.sum(taken(aligned(j * 80), 80).reshape(10, 8, LANES), axis=0)

    amount = lax.fori_loop(0, 25, run, jnp.zeros((8, LANES), jnp.float32))
    amount = jnp.sum(amount, axis=0, keepdims=True) + jnp.sum(taken(2000, 4), axis=0, keepdims=True)
    copies[...] = jnp.broadcast_to(amount[None], (64, 1, LANES))
    shift[...] = top + jnp.log(total)


def quantiles(*args):
    return pl.pallas_call(
        quantile_kernel,
        out_shape=[
            jax.ShapeDtypeStruct((64, 1, LANES), jnp.float32),
            jax.ShapeDtypeStruct((1, LANES), jnp.float32),
        ],
        in_specs=[WHOLE] * 5,
        out_specs=[WHOLE] * 2,
        compiler_params=pltpu.CompilerParams(vmem_limit_bytes=8 << 20),
        cost_estimate=pl.CostEstimate(flops=10 * ROWS * LANES, bytes_accessed=2 * ROWS * LANES * 4, transcendentals=0),
        name="quantiles",
    )(*args)


def step(
    final_activation,
    output_projection_weights,
    context_word_tallies,
    emitted_word_tallies,
    freshest_word,
    recurrence_divisor,
    recurrence_fine,
    appearance_fine,
    softness_level,
    random_draws,
):
    fresh = freshest_word[None]
    emitted = emitted_word_tallies.T

    mine = moved(final_activation, lambda x, y, z, c: (y, x, z, c))
    mine = copies_from(mine, "z")

    def partner(value):
        return moved(value, lambda x, y, z, c: (x, y, z, 1 - c))

    def onward(value):
        return moved(value, lambda x, y, z, c: (x, y + 1 - 2 * c, z, c))

    def backward(value):
        return moved(value, lambda x, y, z, c: (x, y - 1 + 2 * c, z, c))

    other = partner(mine)
    one = onward(mine)
    two = backward(mine)
    weights = fetched(output_projection_weights.T)
    last = onward(one)
    other_one = partner(one)
    other_two = partner(two)
    (parts,) = multiply(first_kernel, 1, [], mine, other, weights)
    (parts,) = multiply(second_kernel, 2, [], one, two, other_one, other_two, weights, parts)
    other_last = partner(last)
    parts, far_a, far_b = multiply(third_kernel, 1, [CODE, CODE], last, other_last, weights, parts)

    far_a = up(far_a)
    far_b = down(far_b)
    after_b, before_a = near(parts)
    b_one, a_one = up(after_b), down(before_a)
    after_a, before_b = relayed(far_a, far_b, parts)
    a_two = up(after_a)
    b_two = down(before_b)
    prepared = early(
        parts,
        a_one,
        b_one,
        context_word_tallies.T,
        emitted,
        fresh,
        recurrence_divisor[None],
        recurrence_fine[None],
        appearance_fine[None],
        softness_level[None],
    )
    scores, local_top, copies = scored(*prepared, a_two, b_two)

    stats = exchanged(copies)
    before, new_counts = prefixes(scores, local_top, emitted, fresh)
    copies, shift = quantiles(stats, local_top, random_draws[None], scores, before)
    sample_quantile = jnp.sum(exchanged(copies), axis=(0, 1))
    log_likelihoods = (scores - shift).T
    return new_counts.T, log_likelihoods, sample_quantile


def solution(mesh):
    split = Mesh(mesh.devices.reshape(NX, NY, NZ, NC), EVERY)
    whole = P("x", PLANE)
    row = P("x")
    return jax.shard_map(
        step,
        mesh=split,
        in_specs=(whole, whole, whole, whole, row, row, row, row, row, row),
        out_specs=(whole, whole, row),
        check_vma=False,
    )
```

```python
import jax
import jax.numpy as jnp
from jax import lax
from jax.experimental import pallas as pl
from jax.experimental.pallas import tpu as pltpu
from jax.sharding import Mesh
from jax.sharding import PartitionSpec as P


VOCAB = 128256
NX, NY, NZ, NC = 4, 4, 8, 2
PLANE = ("y", "z", "c")
EVERY = ("x", "y", "z", "c")

ROWS = 2004
LANES = 128
DEPTH = 2048
HALF = 1008
GROUP = 144
CHUNK = GROUP // 2
STEPS = HALF // GROUP
BLOCKS = ((0, 512), (512, 512), (1024, 512), (1536, ROWS - 1536))
CODED = HALF // 2 + 8
LARGEST = 2**15 - 1

WHOLE = pl.BlockSpec(memory_space=pltpu.VMEM)


def moved(value, to):
    pairs = []
    for x in range(NX):
        for y in range(NY):
            for z in range(NZ):
                for c in range(NC):
                    tx, ty, tz, tc = to(x, y, z, c)
                    source = ((x * NY + y) * NZ + z) * NC + c
                    target = ((tx % NX * NY + ty % NY) * NZ + tz % NZ) * NC + tc % NC
                    pairs.append((source, target))
    return lax.ppermute(value, EVERY, pairs)


def up(value):
    return moved(value, lambda x, y, z, c: (x + 1, y, z, c))


def down(value):
    return moved(value, lambda x, y, z, c: (x - 1, y, z, c))


def copies_from(value, axis):
    size = lax.axis_size(axis)
    copies = jnp.broadcast_to(value, (size, *value.shape))
    return lax.all_to_all(copies, axis, split_axis=0, concat_axis=0, tiled=True)


def exchanged(copies):
    return lax.all_to_all(copies, PLANE, split_axis=0, concat_axis=0, tiled=True)


def step_for(k):
    return jnp.exp2(0.25 * k)


def coded(load, out_ref):
    for group in range(STEPS):
        values = [load(group * GROUP), load(group * GROUP + CHUNK)]
        folded = [value.reshape(CHUNK // 8, 8, LANES) for value in values]
        high = jnp.maximum(jnp.max(folded[0], axis=0), jnp.max(folded[1], axis=0))
        low = jnp.minimum(jnp.min(folded[0], axis=0), jnp.min(folded[1], axis=0))
        high = jnp.max(high, axis=0, keepdims=True)
        low = jnp.min(low, axis=0, keepdims=True)
        middle = 0.5 * (high + low)
        need = jnp.maximum(0.5 * (high - low) * (1.0 / (LARGEST - 1)), jnp.abs(middle) * 2.0**-20)
        k = jnp.ceil(4.0 * jnp.log2(jnp.maximum(need, 1e-30)))
        scale = step_for(-k)
        offset = jnp.round(middle * scale)
        low_word, high_word = (
            jnp.clip(jnp.round(value * scale) - offset, -LARGEST, LARGEST).astype(jnp.int32) for value in values
        )
        out_ref[group * CHUNK : (group + 1) * CHUNK, :] = (low_word & 0xFFFF) | (high_word << 16)
        row = HALF // 2 + group
        out_ref[row : row + 1, :] = (offset.astype(jnp.int32) << 10) | (k.astype(jnp.int32) & 1023)
    out_ref[HALF // 2 + STEPS :, :] = jnp.zeros((8 - STEPS, LANES), jnp.int32)


def decoded(ref, group):
    word = ref[group * CHUNK : (group + 1) * CHUNK, :]
    row = ref[HALF // 2 + group : HALF // 2 + group + 1, :]
    offset = row >> 10
    step = step_for(((row << 22) >> 22).astype(jnp.float32))
    return [(value + offset).astype(jnp.float32) * step for value in ((word << 16) >> 16, word >> 16)]


def aligned(start):
    return pl.multiple_of(start, 8)


def shard_index():
    return (lax.axis_index("y") * NZ + lax.axis_index("z")) * NC + lax.axis_index("c")


def slot_of(r):
    return lax.rem(lax.axis_index("x") + r + NY - lax.axis_index("y"), NY)


def fetch_kernel(source, out, here):
    copies = [
        pltpu.make_async_copy(source.at[pl.ds(start, size)], out.at[pl.ds(start, size)], here.at[n])
        for n, (start, size) in enumerate(BLOCKS)
    ]
    for copy in copies:
        copy.start()
    for copy in copies:
        copy.wait()


def fetched(weights):
    return pl.pallas_call(
        fetch_kernel,
        out_shape=jax.ShapeDtypeStruct(weights.shape, weights.dtype),
        in_specs=[pl.BlockSpec(memory_space=pltpu.HBM)],
        out_specs=WHOLE,
        scratch_shapes=[pltpu.SemaphoreType.DMA((len(BLOCKS),))],
        compiler_params=pltpu.CompilerParams(vmem_limit_bytes=44 << 20),
        cost_estimate=pl.CostEstimate(flops=ROWS * DEPTH * 512, bytes_accessed=ROWS * DEPTH * 4, transcendentals=0),
        name="fetched",
    )(weights)


def lay_out(rows, row, block, core):
    for z in range(NZ):
        at = pl.ds(pl.multiple_of((2 * z + core) * 128, 128), 128)
        rows[pl.ds(pl.multiple_of(row, 128), LANES), at] = block[z]


def multiplied(weights, rows, put):
    for start, size in BLOCKS:
        put(
            start,
            size,
            lax.dot_general(
                weights[pl.ds(start, size), :],
                rows[...],
                (((1,), (1,)), ((), ())),
                preferred_element_type=jnp.float32,
            ),
        )


def clear_tail(parts, slot):
    parts[slot, ROWS : 2 * HALF, :] = jnp.zeros((2 * HALF - ROWS, LANES), jnp.float32)


def first_kernel(mine, other, weights, parts, rows):
    c = lax.axis_index("c")
    lay_out(rows, 0, mine, c)
    lay_out(rows, 0, other, 1 - c)

    def put(start, size, value):
        parts[0, pl.ds(start, size), :] = value

    multiplied(weights, rows, put)
    clear_tail(parts, 0)


def second_kernel(one, two, other_one, other_two, weights, given, parts, rows):
    c = lax.axis_index("c")
    lay_out(rows, c * LANES, one, c)
    lay_out(rows, (1 - c) * LANES, two, c)
    lay_out(rows, (1 - c) * LANES, other_one, 1 - c)
    lay_out(rows, c * LANES, other_two, 1 - c)

    def put(start, size, value):
        parts[3, pl.ds(start, size), :] = value[:, :LANES]
        parts[1, pl.ds(start, size), :] = value[:, LANES:]

    multiplied(weights, rows, put)
    clear_tail(parts, 3)
    clear_tail(parts, 1)


def part_of(parts, r, half):
    slot = slot_of(r)
    return lambda start: parts[slot, pl.ds(aligned(half * HALF + start), CHUNK), :]


def third_kernel(mine, other, weights, given, parts, far_a, far_b, rows):
    c = lax.axis_index("c")
    lay_out(rows, 0, mine, c)
    lay_out(rows, 0, other, 1 - c)

    def put(start, size, value):
        parts[2, pl.ds(start, size), :] = value

    multiplied(weights, rows, put)
    clear_tail(parts, 2)
    coded(part_of(parts, 2, 0), far_a)
    coded(part_of(parts, 2, 1), far_b)


def near_kernel(parts, after_b, before_a):
    coded(part_of(parts, 1, 1), after_b)
    coded(part_of(parts, 3, 0), before_a)


PARTS = jax.ShapeDtypeStruct((NY, 2 * HALF, LANES), jnp.float32)
CODE = jax.ShapeDtypeStruct((CODED, LANES), jnp.int32)


def multiply(kernel, groups, extra, *args):
    given = len(args) - 1 if kernel is not first_kernel else None
    return pl.pallas_call(
        kernel,
        out_shape=[PARTS] + extra,
        in_specs=[WHOLE] * len(args),
        out_specs=[WHOLE] * (1 + len(extra)),
        scratch_shapes=[pltpu.VMEM((groups * LANES, DEPTH), jnp.bfloat16)],
        input_output_aliases={} if given is None else {given: 0},
        compiler_params=pltpu.CompilerParams(vmem_limit_bytes=12 << 20),
        cost_estimate=pl.CostEstimate(
            flops=2 * ROWS * 256 * DEPTH, bytes_accessed=ROWS * DEPTH * 2, transcendentals=0
        ),
    )(*args)


def near(parts):
    return pl.pallas_call(
        near_kernel,
        out_shape=[CODE, CODE],
        in_specs=[WHOLE],
        out_specs=[WHOLE] * 2,
        compiler_params=pltpu.CompilerParams(vmem_limit_bytes=8 << 20),
        cost_estimate=pl.CostEstimate(flops=20 * HALF * LANES, bytes_accessed=4 * HALF * LANES * 4, transcendentals=0),
        name="near",
    )(parts)


def relay_kernel(far_a, far_b, parts, after_out, before_out, total):
    for r, half, far, out in ((1, 0, far_a, after_out), (3, 1, far_b, before_out)):
        own = part_of(parts, r, half)
        for group in range(STEPS):
            for side, value in enumerate(decoded(far, group)):
                start = group * GROUP + side * CHUNK
                total[start : start + CHUNK, :] = own(start) + value
        coded(lambda start: total[start : start + CHUNK, :], out)


def relayed(far_a, far_b, parts):
    return pl.pallas_call(
        relay_kernel,
        out_shape=[CODE, CODE],
        in_specs=[WHOLE] * 3,
        out_specs=[WHOLE] * 2,
        scratch_shapes=[pltpu.VMEM((HALF, LANES), jnp.float32)],
        compiler_params=pltpu.CompilerParams(vmem_limit_bytes=8 << 20),
        cost_estimate=pl.CostEstimate(flops=20 * HALF * LANES, bytes_accessed=4 * HALF * LANES * 4, transcendentals=0),
        name="relayed",
    )(far_a, far_b, parts)


def pieces_of(half, group):
    start = half * HALF + group * GROUP
    return [(side, at, min(CHUNK, ROWS - at)) for side, at in enumerate((start, start + CHUNK))]


def early_kernel(
    parts, a_one, b_one, context, emitted, fresh, divisor, fine, appearance, softness, sums, rising, falling, fines
):
    slot = slot_of(0)
    cooling = 1.0 / softness[...]
    seen_up = cooling / divisor[...]
    seen_down = cooling * divisor[...]
    per_count = fine[...] * cooling
    per_word = appearance[...] * cooling
    newest = fresh[...] - shard_index() * ROWS

    for half, one in ((0, a_one), (1, b_one)):
        for group in range(STEPS):
            values = decoded(one, group)
            for side, start, size in pieces_of(half, group):
                at = pl.ds(start, size)
                sums[at, :] = parts[slot, at, :] + values[side][:size]
                ids = start + lax.broadcasted_iota(jnp.int32, (size, LANES), 0)
                counts = emitted[at, :] + (ids == newest).astype(jnp.int32)
                seen = context[at, :] + counts > 0
                rising[at, :] = jnp.where(seen, seen_up, cooling)
                falling[at, :] = jnp.where(seen, seen_down, cooling)
                fines[at, :] = per_count * counts.astype(jnp.float32) + jnp.where(counts > 0, per_word, 0.0)


def early(*args):
    full = jax.ShapeDtypeStruct((ROWS, LANES), jnp.float32)
    return pl.pallas_call(
        early_kernel,
        out_shape=[full] * 4,
        in_specs=[WHOLE] * 10,
        out_specs=[WHOLE] * 4,
        compiler_params=pltpu.CompilerParams(vmem_limit_bytes=8 << 20),
        cost_estimate=pl.CostEstimate(flops=30 * ROWS * LANES, bytes_accessed=9 * ROWS * LANES * 4, transcendentals=0),
        name="early",
    )(*args)


def scores_kernel(sums, rising, falling, fines, a_two, b_two, scores, line, copies):
    top = jnp.full((8, LANES), -jnp.inf, jnp.float32)
    for half, two in ((0, a_two), (1, b_two)):
        for group in range(STEPS):
            values = decoded(two, group)
            for side, start, size in pieces_of(half, group):
                at = pl.ds(start, size)
                logits = sums[at, :] + values[side][:size]
                score = logits * jnp.where(logits > 0, rising[at, :], falling[at, :]) - fines[at, :]
                scores[at, :] = score
                if size == CHUNK:
                    score = jnp.max(score.reshape(CHUNK // 8, 8, LANES), axis=0)
                else:
                    score = jnp.max(score, axis=0, keepdims=True)
                top = jnp.maximum(top, score)
    top = jnp.max(top, axis=0, keepdims=True)

    def run(j, total):
        value = jnp.exp(scores[pl.ds(aligned(j * 80), 80), :] - top)
        return total + jnp.sum(value.reshape(10, 8, LANES), axis=0)

    total = lax.fori_loop(0, 25, run, jnp.zeros((8, LANES), jnp.float32))
    total = jnp.sum(total, axis=0, keepdims=True)
    total = total + jnp.sum(jnp.exp(scores[2000:ROWS, :] - top), axis=0, keepdims=True)
    line[...] = top
    copies[:, 0:1, :] = jnp.broadcast_to(top[None], (64, 1, LANES))
    copies[:, 1:2, :] = jnp.broadcast_to(total[None], (64, 1, LANES))


def scored(*args):
    full = jax.ShapeDtypeStruct((ROWS, LANES), jnp.float32)
    line = jax.ShapeDtypeStruct((1, LANES), jnp.float32)
    return pl.pallas_call(
        scores_kernel,
        out_shape=[full, line, jax.ShapeDtypeStruct((64, 2, LANES), jnp.float32)],
        in_specs=[WHOLE] * 6,
        out_specs=[WHOLE] * 3,
        compiler_params=pltpu.CompilerParams(vmem_limit_bytes=8 << 20),
        cost_estimate=pl.CostEstimate(flops=30 * ROWS * LANES, bytes_accessed=6 * ROWS * LANES * 4, transcendentals=ROWS * LANES),
        name="scored",
    )(*args)


def prefix_kernel(scores, line, emitted, fresh, before, end, counts):
    newest = fresh[...] - shard_index() * ROWS
    ids = lax.broadcasted_iota(jnp.int32, (8, LANES), 0)
    top = line[...]

    def run(j, carry):
        for t in range(10):
            at = pl.ds(aligned(j * 80 + 8 * t), 8)
            value = jnp.exp(scores[at, :] - top)
            upto = value
            for shift in (1, 2, 4):
                upto = upto + jnp.where(ids >= shift, pltpu.roll(upto, shift, 0), 0.0)
            before[at, :] = (upto - value) + carry
            carry = carry + upto[7:8, :]
            counts[at, :] = emitted[at, :] + (ids + (j * 80 + 8 * t) == newest).astype(jnp.int32)
        return carry

    carry = lax.fori_loop(0, 25, run, jnp.zeros((1, LANES), jnp.float32))
    for row in range(2000, ROWS):
        before[row : row + 1, :] = carry
        carry = carry + jnp.exp(scores[row : row + 1, :] - top)
        counts[row : row + 1, :] = emitted[row : row + 1, :] + (newest == row).astype(jnp.int32)
    end[...] = carry


def prefixes(scores, line, emitted, fresh):
    return pl.pallas_call(
        prefix_kernel,
        out_shape=[
            jax.ShapeDtypeStruct((ROWS, LANES), jnp.float32),
            jax.ShapeDtypeStruct((1, LANES), jnp.float32),
            jax.ShapeDtypeStruct((ROWS, LANES), jnp.int32),
        ],
        in_specs=[WHOLE] * 4,
        out_specs=[WHOLE] * 3,
        compiler_params=pltpu.CompilerParams(vmem_limit_bytes=8 << 20),
        cost_estimate=pl.CostEstimate(flops=400 * ROWS * LANES, bytes_accessed=2 * ROWS * LANES * 4, transcendentals=0),
        name="prefixes",
    )(scores, line, emitted, fresh)


def quantile_kernel(stats, line, draws, before, end, copies, shift):
    shard = shard_index()
    top = jnp.max(stats[...], axis=0)[0:1, :]
    total = jnp.zeros((1, LANES), jnp.float32)
    lower = total
    for peer in range(64):
        part = stats[peer, 1:2, :] * jnp.exp(stats[peer, 0:1, :] - top)
        total = total + part
        lower = lower + jnp.where(peer < shard, part, 0.0)
    share = jnp.exp(line[...] - top) / total
    room = jnp.maximum(draws[...] - lower / total, 0.0)
    whole = jnp.minimum(room, end[...] * share)

    def missing(start, size):
        return whole - jnp.minimum(room, before[pl.ds(start, size), :] * share)

    def run(j, total):
        return total + jnp.sum(missing(aligned(j * 80), 80).reshape(10, 8, LANES), axis=0)

    amount = lax.fori_loop(0, 25, run, jnp.zeros((8, LANES), jnp.float32))
    amount = jnp.sum(amount, axis=0, keepdims=True) + jnp.sum(missing(2000, 4), axis=0, keepdims=True)
    amount = (amount + whole * ((shard * ROWS).astype(jnp.float32) - 0.5)) / VOCAB
    copies[...] = jnp.broadcast_to(amount[None], (64, 1, LANES))
    shift[...] = top + jnp.log(total)


def quantiles(*args):
    return pl.pallas_call(
        quantile_kernel,
        out_shape=[
            jax.ShapeDtypeStruct((64, 1, LANES), jnp.float32),
            jax.ShapeDtypeStruct((1, LANES), jnp.float32),
        ],
        in_specs=[WHOLE] * 5,
        out_specs=[WHOLE] * 2,
        compiler_params=pltpu.CompilerParams(vmem_limit_bytes=8 << 20),
        cost_estimate=pl.CostEstimate(flops=10 * ROWS * LANES, bytes_accessed=2 * ROWS * LANES * 4, transcendentals=0),
        name="quantiles",
    )(*args)


def step(
    final_activation,
    output_projection_weights,
    context_word_tallies,
    emitted_word_tallies,
    freshest_word,
    recurrence_divisor,
    recurrence_fine,
    appearance_fine,
    softness_level,
    random_draws,
):
    fresh = freshest_word[None]
    emitted = emitted_word_tallies.T

    mine = moved(final_activation, lambda x, y, z, c: (y, x, z, c))
    mine = copies_from(mine, "z")

    def partner(value):
        return moved(value, lambda x, y, z, c: (x, y, z, 1 - c))

    def onward(value):
        return moved(value, lambda x, y, z, c: (x, y + 1 - 2 * c, z, c))

    def backward(value):
        return moved(value, lambda x, y, z, c: (x, y - 1 + 2 * c, z, c))

    other = partner(mine)
    one = onward(mine)
    two = backward(mine)
    weights = fetched(output_projection_weights.T)
    last = onward(one)
    other_one = partner(one)
    other_two = partner(two)
    (parts,) = multiply(first_kernel, 1, [], mine, other, weights)
    (parts,) = multiply(second_kernel, 2, [], one, two, other_one, other_two, weights, parts)
    other_last = partner(last)
    parts, far_a, far_b = multiply(third_kernel, 1, [CODE, CODE], last, other_last, weights, parts)

    far_a = up(far_a)
    far_b = down(far_b)
    after_b, before_a = near(parts)
    b_one, a_one = up(after_b), down(before_a)
    after_a, before_b = relayed(far_a, far_b, parts)
    a_two = up(after_a)
    b_two = down(before_b)
    prepared = early(
        parts,
        a_one,
        b_one,
        context_word_tallies.T,
        emitted,
        fresh,
        recurrence_divisor[None],
        recurrence_fine[None],
        appearance_fine[None],
        softness_level[None],
    )
    scores, local_top, copies = scored(*prepared, a_two, b_two)

    stats = exchanged(copies)
    before, end, new_counts = prefixes(scores, local_top, emitted, fresh)
    copies, shift = quantiles(stats, local_top, random_draws[None], before, end)
    sample_quantile = jnp.sum(exchanged(copies), axis=(0, 1))
    log_likelihoods = (scores - shift).T
    return new_counts.T, log_likelihoods, sample_quantile


def solution(mesh):
    split = Mesh(mesh.devices.reshape(NX, NY, NZ, NC), EVERY)
    whole = P("x", PLANE)
    row = P("x")
    return jax.shard_map(
        step,
        mesh=split,
        in_specs=(whole, whole, whole, whole, row, row, row, row, row, row),
        out_specs=(whole, whole, row),
        check_vma=False,
    )
```

```python
import jax
import jax.numpy as jnp
from jax import lax
from jax.experimental import pallas as pl
from jax.experimental.pallas import tpu as pltpu
from jax.sharding import Mesh
from jax.sharding import PartitionSpec as P


VOCAB = 128256
NX, NY, NZ, NC = 4, 4, 8, 2
PLANE = ("y", "z", "c")
EVERY = ("x", "y", "z", "c")

ROWS = 2004
LANES = 128
DEPTH = 2048
HALF = 1008
GROUP = 144
CHUNK = GROUP // 2
STEPS = HALF // GROUP
BLOCKS = ((0, 512), (512, 512), (1024, 512), (1536, ROWS - 1536))
CODED = HALF // 2 + 8
LARGEST = 2**15 - 1

WHOLE = pl.BlockSpec(memory_space=pltpu.VMEM)


def moved(value, to):
    pairs = []
    for x in range(NX):
        for y in range(NY):
            for z in range(NZ):
                for c in range(NC):
                    tx, ty, tz, tc = to(x, y, z, c)
                    source = ((x * NY + y) * NZ + z) * NC + c
                    target = ((tx % NX * NY + ty % NY) * NZ + tz % NZ) * NC + tc % NC
                    pairs.append((source, target))
    return lax.ppermute(value, EVERY, pairs)


def up(value):
    return moved(value, lambda x, y, z, c: (x + 1, y, z, c))


def down(value):
    return moved(value, lambda x, y, z, c: (x - 1, y, z, c))


def copies_from(value, axis):
    size = lax.axis_size(axis)
    copies = jnp.broadcast_to(value, (size, *value.shape))
    return lax.all_to_all(copies, axis, split_axis=0, concat_axis=0, tiled=True)


def exchanged(copies):
    return lax.all_to_all(copies, PLANE, split_axis=0, concat_axis=0, tiled=True)


def step_for(k):
    return jnp.exp2(0.25 * k)


def coded(load, out_ref):
    for group in range(STEPS):
        values = [load(group * GROUP), load(group * GROUP + CHUNK)]
        folded = [value.reshape(CHUNK // 8, 8, LANES) for value in values]
        high = jnp.maximum(jnp.max(folded[0], axis=0), jnp.max(folded[1], axis=0))
        low = jnp.minimum(jnp.min(folded[0], axis=0), jnp.min(folded[1], axis=0))
        high = jnp.max(high, axis=0, keepdims=True)
        low = jnp.min(low, axis=0, keepdims=True)
        middle = 0.5 * (high + low)
        need = jnp.maximum(0.5 * (high - low) * (1.0 / (LARGEST - 1)), jnp.abs(middle) * 2.0**-20)
        k = jnp.ceil(4.0 * jnp.log2(jnp.maximum(need, 1e-30)))
        scale = step_for(-k)
        offset = jnp.round(middle * scale)
        low_word, high_word = (
            jnp.clip(jnp.round(value * scale) - offset, -LARGEST, LARGEST).astype(jnp.int32) for value in values
        )
        out_ref[group * CHUNK : (group + 1) * CHUNK, :] = (low_word & 0xFFFF) | (high_word << 16)
        row = HALF // 2 + group
        out_ref[row : row + 1, :] = (offset.astype(jnp.int32) << 10) | (k.astype(jnp.int32) & 1023)
    out_ref[HALF // 2 + STEPS :, :] = jnp.zeros((8 - STEPS, LANES), jnp.int32)


def decoded(ref, group):
    word = ref[group * CHUNK : (group + 1) * CHUNK, :]
    row = ref[HALF // 2 + group : HALF // 2 + group + 1, :]
    offset = row >> 10
    step = step_for(((row << 22) >> 22).astype(jnp.float32))
    return [(value + offset).astype(jnp.float32) * step for value in ((word << 16) >> 16, word >> 16)]


def aligned(start):
    return pl.multiple_of(start, 8)


def shard_index():
    return (lax.axis_index("y") * NZ + lax.axis_index("z")) * NC + lax.axis_index("c")


def slot_of(r):
    return lax.rem(lax.axis_index("x") + r + NY - lax.axis_index("y"), NY)


def fetch_kernel(source, out, here):
    copies = [
        pltpu.make_async_copy(source.at[pl.ds(start, size)], out.at[pl.ds(start, size)], here.at[n])
        for n, (start, size) in enumerate(BLOCKS)
    ]
    for copy in copies:
        copy.start()
    for copy in copies:
        copy.wait()


def fetched(weights):
    return pl.pallas_call(
        fetch_kernel,
        out_shape=jax.ShapeDtypeStruct(weights.shape, weights.dtype),
        in_specs=[pl.BlockSpec(memory_space=pltpu.HBM)],
        out_specs=WHOLE,
        scratch_shapes=[pltpu.SemaphoreType.DMA((len(BLOCKS),))],
        compiler_params=pltpu.CompilerParams(vmem_limit_bytes=44 << 20),
        cost_estimate=pl.CostEstimate(flops=ROWS * DEPTH * 512, bytes_accessed=ROWS * DEPTH * 4, transcendentals=0),
        name="fetched",
    )(weights)


def lay_out(rows, row, block, core):
    for z in range(NZ):
        at = pl.ds(pl.multiple_of((2 * z + core) * 128, 128), 128)
        rows[pl.ds(pl.multiple_of(row, 128), LANES), at] = block[z]


def multiplied(weights, rows, put):
    for start, size in BLOCKS:
        put(
            start,
            size,
            lax.dot_general(
                weights[pl.ds(start, size), :],
                rows[...],
                (((1,), (1,)), ((), ())),
                preferred_element_type=jnp.float32,
            ),
        )


def clear_tail(parts, slot):
    parts[slot, ROWS : 2 * HALF, :] = jnp.zeros((2 * HALF - ROWS, LANES), jnp.float32)


def first_kernel(mine, other, weights, parts, rows):
    c = lax.axis_index("c")
    lay_out(rows, 0, mine, c)
    lay_out(rows, 0, other, 1 - c)

    def put(start, size, value):
        parts[0, pl.ds(start, size), :] = value

    multiplied(weights, rows, put)
    clear_tail(parts, 0)


def second_kernel(one, two, other_one, other_two, weights, given, parts, rows):
    c = lax.axis_index("c")
    lay_out(rows, c * LANES, one, c)
    lay_out(rows, (1 - c) * LANES, two, c)
    lay_out(rows, (1 - c) * LANES, other_one, 1 - c)
    lay_out(rows, c * LANES, other_two, 1 - c)

    def put(start, size, value):
        parts[3, pl.ds(start, size), :] = value[:, :LANES]
        parts[1, pl.ds(start, size), :] = value[:, LANES:]

    multiplied(weights, rows, put)
    clear_tail(parts, 3)
    clear_tail(parts, 1)


def part_of(parts, r, half):
    slot = slot_of(r)
    return lambda start: parts[slot, pl.ds(aligned(half * HALF + start), CHUNK), :]


def half_kernel(mine, weights, given, parts, rows):
    c = lax.axis_index("c")
    for z in range(NZ):
        rows[:, z * 128 : (z + 1) * 128] = mine[z]
    for start, size in BLOCKS:
        own = jnp.concatenate(
            [weights[pl.ds(start, size), pl.ds(pl.multiple_of((2 * z + c) * 128, 128), 128)] for z in range(NZ)], axis=1
        )
        parts[2, pl.ds(start, size), :] = lax.dot_general(
            own, rows[...], (((1,), (1,)), ((), ())), preferred_element_type=jnp.float32
        )


def third_kernel(other, weights, given, parts, far_a, far_b, rows):
    c = lax.axis_index("c")
    for z in range(NZ):
        rows[:, z * 128 : (z + 1) * 128] = other[z]
    for start, size in BLOCKS:
        theirs = jnp.concatenate(
            [weights[pl.ds(start, size), pl.ds(pl.multiple_of((2 * z + 1 - c) * 128, 128), 128)] for z in range(NZ)],
            axis=1,
        )
        at = pl.ds(start, size)
        parts[2, at, :] = parts[2, at, :] + lax.dot_general(
            theirs, rows[...], (((1,), (1,)), ((), ())), preferred_element_type=jnp.float32
        )
    clear_tail(parts, 2)
    coded(part_of(parts, 2, 0), far_a)
    coded(part_of(parts, 2, 1), far_b)


def near_kernel(parts, after_b, before_a):
    coded(part_of(parts, 1, 1), after_b)
    coded(part_of(parts, 3, 0), before_a)


PARTS = jax.ShapeDtypeStruct((NY, 2 * HALF, LANES), jnp.float32)
CODE = jax.ShapeDtypeStruct((CODED, LANES), jnp.int32)


def multiply(kernel, groups, extra, *args, depth=DEPTH):
    given = len(args) - 1 if kernel is not first_kernel else None
    return pl.pallas_call(
        kernel,
        out_shape=[PARTS] + extra,
        in_specs=[WHOLE] * len(args),
        out_specs=[WHOLE] * (1 + len(extra)),
        scratch_shapes=[pltpu.VMEM((groups * LANES, depth), jnp.bfloat16)],
        input_output_aliases={} if given is None else {given: 0},
        compiler_params=pltpu.CompilerParams(vmem_limit_bytes=12 << 20),
        cost_estimate=pl.CostEstimate(
            flops=2 * ROWS * 256 * DEPTH, bytes_accessed=ROWS * DEPTH * 2, transcendentals=0
        ),
    )(*args)


def near(parts):
    return pl.pallas_call(
        near_kernel,
        out_shape=[CODE, CODE],
        in_specs=[WHOLE],
        out_specs=[WHOLE] * 2,
        compiler_params=pltpu.CompilerParams(vmem_limit_bytes=8 << 20),
        cost_estimate=pl.CostEstimate(flops=20 * HALF * LANES, bytes_accessed=4 * HALF * LANES * 4, transcendentals=0),
        name="near",
    )(parts)


def relay_kernel(far_a, far_b, parts, after_out, before_out, total):
    for r, half, far, out in ((1, 0, far_a, after_out), (3, 1, far_b, before_out)):
        own = part_of(parts, r, half)
        for group in range(STEPS):
            for side, value in enumerate(decoded(far, group)):
                start = group * GROUP + side * CHUNK
                total[start : start + CHUNK, :] = own(start) + value
        coded(lambda start: total[start : start + CHUNK, :], out)


def relayed(far_a, far_b, parts):
    return pl.pallas_call(
        relay_kernel,
        out_shape=[CODE, CODE],
        in_specs=[WHOLE] * 3,
        out_specs=[WHOLE] * 2,
        scratch_shapes=[pltpu.VMEM((HALF, LANES), jnp.float32)],
        compiler_params=pltpu.CompilerParams(vmem_limit_bytes=8 << 20),
        cost_estimate=pl.CostEstimate(flops=20 * HALF * LANES, bytes_accessed=4 * HALF * LANES * 4, transcendentals=0),
        name="relayed",
    )(far_a, far_b, parts)


def pieces_of(half, group):
    start = half * HALF + group * GROUP
    return [(side, at, min(CHUNK, ROWS - at)) for side, at in enumerate((start, start + CHUNK))]


def early_kernel(
    parts, a_one, b_one, context, emitted, fresh, divisor, fine, appearance, softness, sums, rising, falling, fines
):
    slot = slot_of(0)
    cooling = 1.0 / softness[...]
    seen_up = cooling / divisor[...]
    seen_down = cooling * divisor[...]
    per_count = fine[...] * cooling
    per_word = appearance[...] * cooling
    newest = fresh[...] - shard_index() * ROWS

    for half, one in ((0, a_one), (1, b_one)):
        for group in range(STEPS):
            values = decoded(one, group)
            for side, start, size in pieces_of(half, group):
                at = pl.ds(start, size)
                sums[at, :] = parts[slot, at, :] + values[side][:size]
                ids = start + lax.broadcasted_iota(jnp.int32, (size, LANES), 0)
                counts = emitted[at, :] + (ids == newest).astype(jnp.int32)
                seen = context[at, :] + counts > 0
                rising[at, :] = jnp.where(seen, seen_up, cooling)
                falling[at, :] = jnp.where(seen, seen_down, cooling)
                fines[at, :] = per_count * counts.astype(jnp.float32) + jnp.where(counts > 0, per_word, 0.0)


def early(*args):
    full = jax.ShapeDtypeStruct((ROWS, LANES), jnp.float32)
    return pl.pallas_call(
        early_kernel,
        out_shape=[full] * 4,
        in_specs=[WHOLE] * 10,
        out_specs=[WHOLE] * 4,
        compiler_params=pltpu.CompilerParams(vmem_limit_bytes=8 << 20),
        cost_estimate=pl.CostEstimate(flops=30 * ROWS * LANES, bytes_accessed=9 * ROWS * LANES * 4, transcendentals=0),
        name="early",
    )(*args)


def scores_kernel(sums, rising, falling, fines, a_two, b_two, scores, line, copies):
    top = jnp.full((8, LANES), -jnp.inf, jnp.float32)
    for half, two in ((0, a_two), (1, b_two)):
        for group in range(STEPS):
            values = decoded(two, group)
            for side, start, size in pieces_of(half, group):
                at = pl.ds(start, size)
                logits = sums[at, :] + values[side][:size]
                score = logits * jnp.where(logits > 0, rising[at, :], falling[at, :]) - fines[at, :]
                scores[at, :] = score
                if size == CHUNK:
                    score = jnp.max(score.reshape(CHUNK // 8, 8, LANES), axis=0)
                else:
                    score = jnp.max(score, axis=0, keepdims=True)
                top = jnp.maximum(top, score)
    top = jnp.max(top, axis=0, keepdims=True)

    def run(j, total):
        value = jnp.exp(scores[pl.ds(aligned(j * 80), 80), :] - top)
        return total + jnp.sum(value.reshape(10, 8, LANES), axis=0)

    total = lax.fori_loop(0, 25, run, jnp.zeros((8, LANES), jnp.float32))
    total = jnp.sum(total, axis=0, keepdims=True)
    total = total + jnp.sum(jnp.exp(scores[2000:ROWS, :] - top), axis=0, keepdims=True)
    line[...] = top
    copies[:, 0:1, :] = jnp.broadcast_to(top[None], (64, 1, LANES))
    copies[:, 1:2, :] = jnp.broadcast_to(total[None], (64, 1, LANES))


def scored(*args):
    full = jax.ShapeDtypeStruct((ROWS, LANES), jnp.float32)
    line = jax.ShapeDtypeStruct((1, LANES), jnp.float32)
    return pl.pallas_call(
        scores_kernel,
        out_shape=[full, line, jax.ShapeDtypeStruct((64, 2, LANES), jnp.float32)],
        in_specs=[WHOLE] * 6,
        out_specs=[WHOLE] * 3,
        compiler_params=pltpu.CompilerParams(vmem_limit_bytes=8 << 20),
        cost_estimate=pl.CostEstimate(flops=30 * ROWS * LANES, bytes_accessed=6 * ROWS * LANES * 4, transcendentals=ROWS * LANES),
        name="scored",
    )(*args)


def prefix_kernel(scores, line, emitted, fresh, before, end, counts):
    newest = fresh[...] - shard_index() * ROWS
    ids = lax.broadcasted_iota(jnp.int32, (8, LANES), 0)
    top = line[...]

    def run(j, carry):
        for t in range(10):
            at = pl.ds(aligned(j * 80 + 8 * t), 8)
            value = jnp.exp(scores[at, :] - top)
            upto = value
            for shift in (1, 2, 4):
                upto = upto + jnp.where(ids >= shift, pltpu.roll(upto, shift, 0), 0.0)
            before[at, :] = (upto - value) + carry
            carry = carry + upto[7:8, :]
            counts[at, :] = emitted[at, :] + (ids + (j * 80 + 8 * t) == newest).astype(jnp.int32)
        return carry

    carry = lax.fori_loop(0, 25, run, jnp.zeros((1, LANES), jnp.float32))
    for row in range(2000, ROWS):
        before[row : row + 1, :] = carry
        carry = carry + jnp.exp(scores[row : row + 1, :] - top)
        counts[row : row + 1, :] = emitted[row : row + 1, :] + (newest == row).astype(jnp.int32)
    end[...] = carry


def prefixes(scores, line, emitted, fresh):
    return pl.pallas_call(
        prefix_kernel,
        out_shape=[
            jax.ShapeDtypeStruct((ROWS, LANES), jnp.float32),
            jax.ShapeDtypeStruct((1, LANES), jnp.float32),
            jax.ShapeDtypeStruct((ROWS, LANES), jnp.int32),
        ],
        in_specs=[WHOLE] * 4,
        out_specs=[WHOLE] * 3,
        compiler_params=pltpu.CompilerParams(vmem_limit_bytes=8 << 20),
        cost_estimate=pl.CostEstimate(flops=400 * ROWS * LANES, bytes_accessed=2 * ROWS * LANES * 4, transcendentals=0),
        name="prefixes",
    )(scores, line, emitted, fresh)


def quantile_kernel(stats, line, draws, before, end, copies, shift):
    shard = shard_index()
    top = jnp.max(stats[...], axis=0)[0:1, :]
    total = jnp.zeros((1, LANES), jnp.float32)
    lower = total
    for peer in range(64):
        part = stats[peer, 1:2, :] * jnp.exp(stats[peer, 0:1, :] - top)
        total = total + part
        lower = lower + jnp.where(peer < shard, part, 0.0)
    share = jnp.exp(line[...] - top) / total
    room = jnp.maximum(draws[...] - lower / total, 0.0)
    whole = jnp.minimum(room, end[...] * share)

    def missing(start, size):
        return whole - jnp.minimum(room, before[pl.ds(start, size), :] * share)

    def run(j, total):
        return total + jnp.sum(missing(aligned(j * 80), 80).reshape(10, 8, LANES), axis=0)

    amount = lax.fori_loop(0, 25, run, jnp.zeros((8, LANES), jnp.float32))
    amount = jnp.sum(amount, axis=0, keepdims=True) + jnp.sum(missing(2000, 4), axis=0, keepdims=True)
    amount = (amount + whole * ((shard * ROWS).astype(jnp.float32) - 0.5)) / VOCAB
    copies[...] = jnp.broadcast_to(amount[None], (64, 1, LANES))
    shift[...] = top + jnp.log(total)


def quantiles(*args):
    return pl.pallas_call(
        quantile_kernel,
        out_shape=[
            jax.ShapeDtypeStruct((64, 1, LANES), jnp.float32),
            jax.ShapeDtypeStruct((1, LANES), jnp.float32),
        ],
        in_specs=[WHOLE] * 5,
        out_specs=[WHOLE] * 2,
        compiler_params=pltpu.CompilerParams(vmem_limit_bytes=8 << 20),
        cost_estimate=pl.CostEstimate(flops=10 * ROWS * LANES, bytes_accessed=2 * ROWS * LANES * 4, transcendentals=0),
        name="quantiles",
    )(*args)


def step(
    final_activation,
    output_projection_weights,
    context_word_tallies,
    emitted_word_tallies,
    freshest_word,
    recurrence_divisor,
    recurrence_fine,
    appearance_fine,
    softness_level,
    random_draws,
):
    fresh = freshest_word[None]
    emitted = emitted_word_tallies.T

    mine = moved(final_activation, lambda x, y, z, c: (y, x, z, c))
    mine = copies_from(mine, "z")

    def partner(value):
        return moved(value, lambda x, y, z, c: (x, y, z, 1 - c))

    def onward(value):
        return moved(value, lambda x, y, z, c: (x, y + 1 - 2 * c, z, c))

    def backward(value):
        return moved(value, lambda x, y, z, c: (x, y - 1 + 2 * c, z, c))

    other = partner(mine)
    one = onward(mine)
    two = backward(mine)
    weights = fetched(output_projection_weights.T)
    last = onward(one)
    other_one = partner(one)
    other_two = partner(two)
    (parts,) = multiply(first_kernel, 1, [], mine, other, weights)
    (parts,) = multiply(second_kernel, 2, [], one, two, other_one, other_two, weights, parts)
    other_last = partner(last)
    (parts,) = multiply(half_kernel, 1, [], last, weights, parts, depth=DEPTH // 2)
    parts, far_a, far_b = multiply(third_kernel, 1, [CODE, CODE], other_last, weights, parts, depth=DEPTH // 2)

    far_a = up(far_a)
    far_b = down(far_b)
    after_b, before_a = near(parts)
    b_one, a_one = up(after_b), down(before_a)
    after_a, before_b = relayed(far_a, far_b, parts)
    a_two = up(after_a)
    b_two = down(before_b)
    prepared = early(
        parts,
        a_one,
        b_one,
        context_word_tallies.T,
        emitted,
        fresh,
        recurrence_divisor[None],
        recurrence_fine[None],
        appearance_fine[None],
        softness_level[None],
    )
    scores, local_top, copies = scored(*prepared, a_two, b_two)

    stats = exchanged(copies)
    before, end, new_counts = prefixes(scores, local_top, emitted, fresh)
    copies, shift = quantiles(stats, local_top, random_draws[None], before, end)
    sample_quantile = jnp.sum(exchanged(copies), axis=(0, 1))
    log_likelihoods = (scores - shift).T
    return new_counts.T, log_likelihoods, sample_quantile


def solution(mesh):
    split = Mesh(mesh.devices.reshape(NX, NY, NZ, NC), EVERY)
    whole = P("x", PLANE)
    row = P("x")
    return jax.shard_map(
        step,
        mesh=split,
        in_specs=(whole, whole, whole, whole, row, row, row, row, row, row),
        out_specs=(whole, whole, row),
        check_vma=False,
    )
```
